128 devices in a mesh: tp: 2 (over core), ep: 64 (over z, y, x).
Axes of the slice: x: 4, y: 4, z: 4, core: 2. Of those that a mesh axis runs over, the one named last changes fastest.
Arguments:
- x: bfloat16 [32768, 2048], P(('ep', 'tp'))
- idx: int32 [32768, 6], P(('ep', 'tp'))
- g: float32 [32768, 6], P(('ep', 'tp'))
- slot: int32 [32768, 6], P(('ep', 'tp'))
- ws1: bfloat16 [2048, 2816], P(None, 'tp')
- ws3: bfloat16 [2048, 2816], P(None, 'tp')
- ws2: bfloat16 [2816, 2048], P('tp')
- w1: bfloat16 [64, 2048, 1408], P('ep')
- w3: bfloat16 [64, 2048, 1408], P('ep')
- w2: bfloat16 [64, 1408, 2048], P('ep')
Outputs:
- output: bfloat16 [32768, 2048], P(('ep', 'tp'))
All inputs are finite; a program needn't handle non-finite values.
Results may differ from the reference program's by a relative error of at most 0.001.
Values are sent between devices in bfloat16 or wider.
A program may use at most 1 GiB of HBM per device.

```python
import jax
import jax.numpy as jnp
from jax import lax

D = 2048
F = 1408
FS = 2816
E = 64
K = 6
TOK = 256
DEV = 128
C = 48

T = TOK * DEV
ROWS = DEV * C


def _weights(key, n, shape, fan_in):
    return lax.map(lambda kk: (jax.random.normal(kk, shape, jnp.float32) * fan_in ** -0.5).astype(jnp.bfloat16), jax.random.split(key, n))


def _positions(idx):
    oh = jax.nn.one_hot(idx.reshape(DEV, TOK * K), E, dtype=jnp.int32)
    return jnp.sum((jnp.cumsum(oh, axis=1) - 1) * oh, axis=-1).reshape(T, K)


def _route_ids(key):
    weight = jnp.uint32(96) + (jnp.uint32(256) * jnp.arange(E, dtype=jnp.uint32)) // jnp.uint32(E)
    wait = (jax.random.bits(key, (T, E), jnp.uint32) >> 10) * weight[None, :]
    return jnp.argsort(wait, axis=-1, stable=True)[:, :K].astype(jnp.int32)


def setup_inputs(seed: int = 0) -> dict:
    ks = jax.random.split(jax.random.PRNGKey(seed), 10)
    x = jax.random.normal(ks[0], (T, D), jnp.float32).astype(jnp.bfloat16)
    idx = _route_ids(jax.random.fold_in(ks[1], 7))
    g = jax.random.uniform(ks[2], (T, K), jnp.float32, 0.4, 1.0)
    pos = _positions(idx)
    slot = jnp.where(pos < C, C - 1 - pos, -1).astype(jnp.int32)
    return {
        "x": x, "idx": idx, "g": g, "slot": slot,
        "ws1": _weights(ks[3], 1, (D, FS), D)[0],
        "ws3": _weights(ks[4], 1, (D, FS), D)[0],
        "ws2": _weights(ks[5], 1, (FS, D), FS)[0],
        "w1": _weights(ks[6], E, (D, F), D),
        "w3": _weights(ks[7], E, (D, F), D),
        "w2": _weights(ks[8], E, (F, D), F),
    }


def _swiglu(x, w1, w3, w2):
    a = jnp.dot(x, w1, preferred_element_type=jnp.float32)
    b = jnp.dot(x, w3, preferred_element_type=jnp.float32)
    h = (jax.nn.silu(a) * b).astype(jnp.bfloat16)
    return jnp.dot(h, w2, preferred_element_type=jnp.float32)


def reference(x, idx, g, slot, ws1, ws3, ws2, w1, w3, w2):
    s = _swiglu(x, ws1, ws3, ws2)
    blk = (jnp.arange(T, dtype=jnp.int32) // TOK)[:, None]
    kept = slot >= 0
    dest = jnp.where(kept, idx * ROWS + blk * C + slot, E * ROWS)
    buf = jnp.zeros((E * ROWS, D), jnp.bfloat16)
    for j in range(K):
        buf = buf.at[dest[:, j]].set(x, mode="drop")
    out = lax.map(lambda a: _swiglu(*a).astype(jnp.bfloat16), (buf.reshape(E, ROWS, D), w1, w3, w2))
    out = out.reshape(E * ROWS, D)
    gate = jnp.where(kept, g, 0.0)
    src = jnp.where(kept, dest, 0)
    y = x.astype(jnp.float32) + s
    for j in range(K):
        y = y + gate[:, j:j + 1] * jnp.take(out, src[:, j], axis=0).astype(jnp.float32)
    return y.astype(jnp.bfloat16)
```

```python
import jax
import jax.numpy as jnp
from jax import lax
from jax.experimental import pallas as pl
from jax.experimental.pallas import tpu as pltpu
from jax.sharding import PartitionSpec as P

MESH = pl.DeviceIdType.MESH
BF = jnp.bfloat16
F32 = jnp.float32

TOK = 256
D = 2048
F = 1408
K = 6
CAP = 48
CH = 16
NC = CAP // CH
NT = F // 128

COLS = ((0, 640), (640, 640), (1280, 768))
ORDER = ((0, 1, 2), (2, 0, 1), (1, 2, 0))
D1, PS, D2, D3, R3, R2, R1 = range(7)
BASE = {D1: 0, PS: 9, D2: 18, D3: 45, R3: 72, R2: 99, R1: 126}
NSEM = 126 + 108


def _sem(stage, c, p, i, k=0):
    if stage == R1:
        return BASE[R1] + ((c * 3 + p) * 3 + i - 1) * 4 + k
    return BASE[stage] + (c * 3 + p) * 3 + i - 1


def _kernel(x, post, posn, gn, ws1, ws3, ws2, w1, w3, w2,
            out, sa, sb, sc, e, q3a, q3b, q3c, q2a, q2b, q2c, h,
            la, lb, lc, pt, pa, pb, pc, ec, hc, r, w13, w2v, hid, gm,
            acc, xs, part, prem, ssem, rsem, lsem, wsem, tsem):
    ep = lax.axis_index("ep")
    tp = lax.axis_index("tp")
    m = (ep // 16, (ep // 4) % 4, ep % 4)
    mz, my, mx = m
    s = (sa, sb, sc)
    q3 = (q3a, q3b, q3c)
    q2 = (q2a, q2b, q2c)
    line = (la, lb, lc)
    pk = (pa, pb, pc)
    cols = tuple(pl.ds(a, b) for a, b in COLS)

    def dev(d, i):
        t = [mz, my, mx]
        t[d] = (t[d] + i) % 4
        return {"ep": t[0] * 16 + t[1] * 4 + t[2]}

    def at(d, i):
        return (m[d] + i) % 4

    def src(d, i):
        return (m[d] + 4 - i) % 4

    def weights(u1, u3, u2):
        cps = []
        for n in range(NT):
            cps.append(pltpu.make_async_copy(u1.at[:, pl.ds(n * 128, 128)], w13.at[n, :, pl.ds(0, 128)], wsem.at[2 * n]))
            cps.append(pltpu.make_async_copy(u3.at[:, pl.ds(n * 128, 128)], w13.at[n, :, pl.ds(128, 128)], wsem.at[2 * n + 1]))
        for n in range(8):
            cps.append(pltpu.make_async_copy(u2.at[:, pl.ds(n * 256, 256)], w2v.at[n], wsem.at[2 * NT + n]))
        return cps

    wshared = weights(ws1, ws3, ws2)
    for c in wshared:
        c.start()
    own_x = pltpu.make_async_copy(x, xs.at[0], lsem.at[0])
    own_x.start()
    own_line = [pltpu.make_async_copy(x.at[:, cols[p]], line[p].at[m[ORDER[p][0]]], lsem.at[1 + p]) for p in range(3)]
    for c in own_line:
        c.start()

    bar = pltpu.get_barrier_semaphore()
    for d in range(3):
        for i in range(1, 4):
            pl.semaphore_signal(bar, inc=1, device_id=dev(d, i), device_id_type=MESH)
    pl.semaphore_signal(bar, inc=1, device_id={"tp": 1 - tp}, device_id_type=MESH)
    pl.semaphore_wait(bar, 10)

    sent = []

    def remote(a, b, stage, c, p, i, where, k=0):
        n = _sem(stage, c, p, i, k)
        cp = pltpu.make_async_remote_copy(src_ref=a, dst_ref=b, send_sem=ssem.at[n], recv_sem=rsem.at[n],
                                          device_id=where, device_id_type=MESH)
        cp.start()
        sent.append(cp)
        return cp

    d1 = []
    for i in (1, 3, 2):
        for p in range(3):
            d = ORDER[p][0]
            d1.append(remote(post, pt.at[d, m[d]], PS, 0, p, i, dev(d, i)))
            d1.append(remote(x.at[:, cols[p]], line[p].at[m[d]], D1, 0, p, i, dev(d, i)))
    xcp = pltpu.make_async_remote_copy(src_ref=x, dst_ref=xs.at[1], send_sem=tsem.at[0], recv_sem=tsem.at[1],
                                       device_id={"tp": 1 - tp}, device_id_type=MESH)
    xcp.start()
    for d in range(3):
        pt[d, m[d]] = post[...]

    def up(rows):
        def body(n, _):
            ab = jnp.dot(rows(), w13[n], preferred_element_type=F32)
            a = ab[:, :128]
            hid[:, pl.ds(pl.multiple_of(n * 128, 128), 128)] = (jax.nn.silu(a) * ab[:, 128:]).astype(BF)
            return 0
        lax.fori_loop(0, NT, body, 0)

    def down(store):
        def body(n, _):
            store(n, jnp.dot(hid[...], w2v[n], preferred_element_type=F32))
            return 0
        lax.fori_loop(0, 8, body, 0)

    def col(n):
        return pl.ds(pl.multiple_of(n * 256, 256), 256)

    own_x.wait()
    for c in wshared:
        c.wait()
    up(lambda: xs[0])

    def own_rows(n, v):
        acc[:, col(n)] = xs[0, :, col(n)].astype(F32) + v
    down(own_rows)

    for c in own_line:
        c.wait()
    for c in d1:
        c.wait_recv()

    ri = lax.broadcasted_iota(jnp.int32, (TOK, TOK), 0)
    ra, rb, rs = ri // 64, (ri // 16) % 4, ri % 16
    ex = (mz * 16 + ra * 4 + rb, ra * 16 + rb * 4 + mx, rb * 16 + my * 4 + ra)

    def pack(c):
        for p in range(3):
            d = ORDER[p][0]
            tgt = ex[p] * CAP + (rs + c * CH)

            def body(k, _, p=p, d=d, tgt=tgt):
                ps = pt[d, k]
                hit = ps[0:1, :] == tgt
                for j in range(1, K):
                    hit = hit | (ps[j:j + 1, :] == tgt)
                oh = jnp.where(hit, 1.0, 0.0).astype(BF)
                v = jnp.dot(oh, line[p][k], preferred_element_type=F32).astype(BF)
                pk[p][c % 2, :, :, k] = v.reshape(4, 4, CH, COLS[p][1])
                return 0
            lax.fori_loop(0, 4, body, 0)

    def s_dst(p, c, b):
        return s[p].at[c, :, b] if p == 1 else s[p].at[c, :, :, b]

    def send_d2(c):
        res = []
        for i in (1, 3, 2):
            for p in range(3):
                d = ORDER[p][1]
                res.append(remote(pk[p].at[c % 2, at(d, i)], s_dst(p, c, m[d]), D2, c, p, i, dev(d, i)))
        loc = []
        for p in range(3):
            d = ORDER[p][1]
            cp = pltpu.make_async_copy(pk[p].at[c % 2, m[d]], s_dst(p, c, m[d]), lsem.at[4 + c * 3 + p])
            cp.start()
            loc.append(cp)
        return res, loc

    def e_at(buf, p, v):
        if p == 0:
            return buf.at[:, :, v, :, cols[0]]
        if p == 1:
            return buf.at[:, v, :, :, cols[1]]
        return buf.at[v, :, :, :, cols[2]]

    def send_d3(c):
        res = []
        for i in (1, 3, 2):
            for p in range(3):
                d = ORDER[p][2]
                res.append(remote(s[p].at[c, at(d, i)], e_at(e.at[c], p, m[d]), D3, c, p, i, dev(d, i)))
        return res

    def load_e(c):
        cps = []
        for p in range(3):
            d = ORDER[p][2]
            cps.append(pltpu.make_async_copy(s[p].at[c, m[d]], e_at(ec, p, m[d]), lsem.at[13 + p * 4]))
            for i in range(1, 4):
                v = src(d, i)
                cps.append(pltpu.make_async_copy(e_at(e.at[c], p, v), e_at(ec, p, v), lsem.at[13 + p * 4 + i]))
        for cp in cps:
            cp.start()
        for cp in cps:
            cp.wait()

    def experts(c, z):
        up(lambda: ec[z].reshape(TOK, D))

        def store(n, v):
            r[c % 2, z, :, :, :, col(n)] = v.astype(BF).reshape(4, 4, CH, 256)
        down(store)

    def send_r3(c):
        res, loc = [], []
        for i in (1, 3, 2):
            for p in range(3):
                d = ORDER[p][2]
                res.append(remote(e_at(r.at[c % 2], p, at(d, i)), q3[p].at[c, m[d]], R3, c, p, i, dev(d, i)))
        for p in range(3):
            d = ORDER[p][2]
            cp = pltpu.make_async_copy(e_at(r.at[c % 2], p, m[d]), q3[p].at[c, m[d]], lsem.at[25 + c * 3 + p])
            cp.start()
            loc.append(cp)
        return res, loc

    def q3_at(p, c, v):
        return q3[p].at[c, :, v] if p == 1 else q3[p].at[c, :, :, v]

    def q2_at(p, c, v):
        return q2[p].at[c, :, v] if p == 2 else q2[p].at[c, v]

    def send_r2(c):
        res = []
        for i in (1, 3, 2):
            for p in range(3):
                d = ORDER[p][1]
                res.append(remote(q3_at(p, c, at(d, i)), q2_at(p, c, m[d]), R2, c, p, i, dev(d, i)))
        return res

    def r1_src(p, c, v, w, own):
        if p == 0:
            return q3a.at[c, :, v, w] if own else q2a.at[c, w, :, v]
        if p == 1:
            return q3b.at[c, :, w, v] if own else q2b.at[c, w, :, v]
        return q3c.at[c, :, v, w] if own else q2c.at[c, :, w, v]

    def h_at(buf, p, v, w):
        if p == 0:
            return buf.at[v, w, :, :, cols[0]]
        if p == 1:
            return buf.at[w, :, v, :, cols[1]]
        return buf.at[:, v, w, :, cols[2]]

    def send_r1(c):
        res = []
        for i in (1, 3, 2):
            for k in range(4):
                for p in range(3):
                    d, d2 = ORDER[p][0], ORDER[p][1]
                    w = src(d2, k)
                    res.append(remote(r1_src(p, c, at(d, i), w, k == 0), h_at(h.at[c], p, m[d], w),
                                      R1, c, p, i, dev(d, i), k))
        return res

    def load_h(c):
        cps = []
        n = 34
        for p in range(3):
            d, d2 = ORDER[p][0], ORDER[p][1]
            for k in range(4):
                w = src(d2, k)
                cps.append(pltpu.make_async_copy(r1_src(p, c, m[d], w, k == 0), h_at(hc, p, m[d], w), lsem.at[n]))
                n += 1
            for i in range(1, 4):
                v = src(d, i)
                if p == 0:
                    a, b = h.at[c, v, :, :, :, cols[0]], hc.at[v, :, :, :, cols[0]]
                elif p == 1:
                    a, b = h.at[c, :, :, v, :, cols[1]], hc.at[:, :, v, :, cols[1]]
                else:
                    a, b = h.at[c, :, v, :, :, cols[2]], hc.at[:, v, :, :, cols[2]]
                cps.append(pltpu.make_async_copy(a, b, lsem.at[n]))
                n += 1
        for cp in cps:
            cp.start()
        for cp in cps:
            cp.wait()

    li = lax.broadcasted_iota(jnp.int32, (TOK, TOK), 1)

    def combine(c):
        def zz(z, _):
            tgt = (z * 16 + li // 16) * CAP + (li % 16 + c * CH)
            g = jnp.zeros((TOK, TOK), F32)
            for j in range(K):
                g = g + jnp.where(posn[:, j:j + 1] == tgt, gn[:, j:j + 1], 0.0)
            g1 = g.astype(BF)
            t = g - g1.astype(F32)
            g2 = t.astype(BF)
            gm[0] = g1
            gm[1] = g2
            gm[2] = (t - g2.astype(F32)).astype(BF)

            def body(n, _):
                b = hc[z, :, :, :, col(n)].reshape(TOK, 256)
                v = jnp.dot(gm[2], b, preferred_element_type=F32)
                v = v + jnp.dot(gm[1], b, preferred_element_type=F32)
                v = v + jnp.dot(gm[0], b, preferred_element_type=F32)
                acc[:, col(n)] = acc[:, col(n)] + v
                return 0
            lax.fori_loop(0, 8, body, 0)
            return 0
        lax.fori_loop(0, 4, zz, 0)

    def got(res):
        for cp in res:
            cp.wait_recv()

    def loop(lo, hi, f):
        def body(z, _):
            f(z)
            return 0
        lax.fori_loop(lo, hi, body, 0)

    pack(0)
    d20, l20 = send_d2(0)
    pack(1)
    d21, l21 = send_d2(1)

    xcp.wait()
    up(lambda: xs[1])

    def other_rows(n, v):
        part[:, col(n)] = v
    down(other_rows)
    pcp = pltpu.make_async_remote_copy(src_ref=part, dst_ref=prem, send_sem=tsem.at[2], recv_sem=tsem.at[3],
                                       device_id={"tp": 1 - tp}, device_id_type=MESH)
    pcp.start()
    wexp = weights(w1.at[0], w3.at[0], w2.at[0])
    for c in wexp:
        c.start()

    got(d20)
    for c in l20:
        c.wait()
    d30 = send_d3(0)
    for c in d20:
        c.wait_send()
    pack(2)
    d22, l22 = send_d2(2)
    got(d21)
    for c in l21:
        c.wait()
    d31 = send_d3(1)
    for c in wexp:
        c.wait()

    got(d30)
    load_e(0)
    loop(0, 4, lambda z: experts(0, z))
    got(d22)
    for c in l22:
        c.wait()
    d32 = send_d3(2)
    r30, k30 = send_r3(0)

    got(d31)
    load_e(1)
    loop(0, 4, lambda z: experts(1, z))
    r31, k31 = send_r3(1)

    got(d32)
    load_e(2)
    for c in r30:
        c.wait_send()
    for c in k30:
        c.wait()
    loop(0, 2, lambda z: experts(2, z))
    got(r30)
    r20 = send_r2(0)
    loop(2, 4, lambda z: experts(2, z))
    r32, k32 = send_r3(2)

    got(r31)
    for c in k31:
        c.wait()
    r21 = send_r2(1)
    got(r20)
    r10 = send_r1(0)
    got(r32)
    for c in k32:
        c.wait()
    r22 = send_r2(2)
    got(r21)
    r11 = send_r1(1)
    got(r10)
    load_h(0)
    combine(0)
    got(r22)
    r12 = send_r1(2)
    got(r11)
    load_h(1)
    combine(1)
    pcp.wait()
    acc[...] = acc[...] + prem[...]
    got(r12)
    load_h(2)
    combine(2)
    out[...] = acc[...].astype(BF)
    done = set(id(c) for c in d20 + r30)
    for c in sent:
        if id(c) not in done:
            c.wait_send()


def _layer(x, post, posn, gn, ws1, ws3, ws2, w1, w3, w2):
    any_ = pl.BlockSpec(memory_space=pl.ANY)
    vm = pl.BlockSpec(memory_space=pltpu.VMEM)

    def blk(n):
        return jax.ShapeDtypeStruct((NC, 4, 4, 4, CH, n), BF)
    per = [blk(b) for _, b in COLS]
    shapes = [jax.ShapeDtypeStruct((TOK, D), BF)] + per + [blk(D)] + per + per + [blk(D)]
    scratch = [pltpu.VMEM((4, TOK, b), BF) for _, b in COLS]
    scratch += [pltpu.VMEM((3, 4, 8, TOK), jnp.int32)]
    scratch += [pltpu.VMEM((2, 4, 4, 4, CH, b), BF) for _, b in COLS]
    scratch += [
        pltpu.VMEM((4, 4, 4, CH, D), BF),
        pltpu.VMEM((4, 4, 4, CH, D), BF),
        pltpu.VMEM((2, 4, 4, 4, CH, D), BF),
        pltpu.VMEM((NT, D, 256), BF),
        pltpu.VMEM((8, F, 256), BF),
        pltpu.VMEM((TOK, F), BF),
        pltpu.VMEM((3, TOK, TOK), BF),
        pltpu.VMEM((TOK, D), F32),
        pltpu.VMEM((2, TOK, D), BF),
        pltpu.VMEM((TOK, D), F32),
        pltpu.VMEM((TOK, D), F32),
        pltpu.SemaphoreType.DMA((NSEM,)),
        pltpu.SemaphoreType.DMA((NSEM,)),
        pltpu.SemaphoreType.DMA((55,)),
        pltpu.SemaphoreType.DMA((2 * NT + 8,)),
        pltpu.SemaphoreType.DMA((4,)),
    ]
    return pl.pallas_call(
        _kernel,
        out_shape=shapes,
        in_specs=[any_, vm, vm, vm] + [any_] * 6,
        out_specs=[vm] + [any_] * (len(shapes) - 1),
        scratch_shapes=scratch,
        compiler_params=pltpu.CompilerParams(collective_id=0, has_side_effects=True, vmem_limit_bytes=67043328),
    )(x, post, posn, gn, ws1, ws3, ws2, w1, w3, w2)[0]


def solution(mesh):
    rows = P(("ep", "tp"), None)

    def body(x, idx, g, slot, ws1, ws3, ws2, w1, w3, w2):
        pos = jnp.where(slot >= 0, idx * CAP + slot, -1)
        posn = jnp.pad(pos, ((0, 0), (0, 2)), constant_values=-1)
        gn = jnp.pad(g, ((0, 0), (0, 2)))
        return _layer(x, posn.T, posn, gn, ws1, ws3, ws2, w1, w3, w2)

    return jax.shard_map(
        body, mesh=mesh,
        in_specs=(rows, rows, rows, rows, P(None, "tp"), P(None, "tp"), P("tp", None),
                  P("ep", None, None), P("ep", None, None), P("ep", None, None)),
        out_specs=rows, check_vma=False)
```

```python
import jax
import jax.numpy as jnp
from jax import lax
from jax.experimental import pallas as pl
from jax.experimental.pallas import tpu as pltpu
from jax.sharding import PartitionSpec as P

MESH = pl.DeviceIdType.MESH
BF = jnp.bfloat16
F32 = jnp.float32

TOK = 256
D = 2048
F = 1408
K = 6
CAP = 48
CH = 16
NC = CAP // CH
NT = F // 128

COLS = ((0, 640), (640, 640), (1280, 768))
ORDER = ((0, 1, 2), (2, 0, 1), (1, 2, 0))
D1, PS, GS, R1, D2, D3, R3, R2 = range(8)
BASE = {D1: 0, PS: 9, GS: 18, R1: 27, D3: 36, R3: 63, R2: 90, D2: 117}
NSEM = 117 + 108


def _sem(stage, c, p, i, k):
    if stage == D2:
        return BASE[D2] + ((c * 3 + p) * 3 + i - 1) * 4 + k
    return BASE[stage] + (c * 3 + p) * 3 + i - 1


def _kernel(x, idx, slot, g, ws1, ws3, ws2, w1, w3, w2,
            own, sa, sb, sc, e, q3a, q3b, q3c, q2a, q2b, q2c, fr,
            la, lb, lc, pt, gt, pm, gm, wt, pa, pb, pc, oa, ob, oc, ec, qa, qb, qc, r, w13, w2v, hid,
            acc, xs, prem, ssem, rsem, lsem, wsem, tsem):
    ep = lax.axis_index("ep")
    tp = lax.axis_index("tp")
    m = (ep // 16, (ep // 4) % 4, ep % 4)
    mz, my, mx = m
    s = (sa, sb, sc)
    q3 = (q3a, q3b, q3c)
    q2 = (q2a, q2b, q2c)
    line = (la, lb, lc)
    pk = (pa, pb, pc)
    po = (oa, ob, oc)
    qv = (qa, qb, qc)
    cols = tuple(pl.ds(a, b) for a, b in COLS)

    def dev(d, i):
        t = [mz, my, mx]
        t[d] = (t[d] + i) % 4
        return {"ep": t[0] * 16 + t[1] * 4 + t[2]}

    def at(d, i):
        return (m[d] + i) % 4

    def src(d, i):
        return (m[d] + 4 - i) % 4

    def weights(u1, u3, u2):
        cps = []
        for n in range(NT):
            cps.append(pltpu.make_async_copy(u1.at[:, pl.ds(n * 128, 128)], w13.at[n, :, pl.ds(0, 128)], wsem.at[2 * n]))
            cps.append(pltpu.make_async_copy(u3.at[:, pl.ds(n * 128, 128)], w13.at[n, :, pl.ds(128, 128)], wsem.at[2 * n + 1]))
        for n in range(8):
            cps.append(pltpu.make_async_copy(u2.at[:, pl.ds(n * 256, 256)], w2v.at[n], wsem.at[2 * NT + n]))
        return cps

    bar = pltpu.get_barrier_semaphore()
    for d in range(3):
        for i in range(1, 4):
            pl.semaphore_signal(bar, inc=1, device_id=dev(d, i), device_id_type=MESH)
    pl.semaphore_signal(bar, inc=1, device_id={"tp": 1 - tp}, device_id_type=MESH)

    own_x = pltpu.make_async_copy(x, xs.at[0], lsem.at[0])
    own_x.start()
    own_line = [pltpu.make_async_copy(x.at[:, cols[p]], line[p].at[m[ORDER[p][0]]], lsem.at[1 + p]) for p in range(3)]
    for c in own_line:
        c.start()
    pm[...] = jnp.full((8, TOK), -1, jnp.int32)
    gm[...] = jnp.zeros((8, TOK), F32)
    pm[0:K, :] = jnp.where(slot[...] >= 0, idx[...] * CAP + slot[...], -1)
    gm[0:K, :] = g[...]
    for d in range(3):
        pt[d, m[d]] = pm[...]
        gt[d, m[d]] = gm[...]
    pl.semaphore_wait(bar, 10)

    def remote(a, b, stage, c, p, i, where, k=0):
        n = _sem(stage, c, p, i, k)
        return pltpu.make_async_remote_copy(src_ref=a, dst_ref=b, send_sem=ssem.at[n], recv_sem=rsem.at[n],
                                            device_id=where, device_id_type=MESH)

    def local(a, b, n):
        return pltpu.make_async_copy(a, b, lsem.at[n])

    def go(cps):
        for cp in cps:
            cp.start()

    def fin(cps):
        for cp in cps:
            cp.wait()

    def got(cps):
        for cp in cps:
            cp.wait_recv()

    def gone(cps):
        for cp in cps:
            cp.wait_send()

    near = (1, 3, 2)

    d1 = []
    for i in near:
        for p in range(3):
            d = ORDER[p][0]
            d1.append(remote(pm, pt.at[d, m[d]], PS, 0, p, i, dev(d, i)))
            d1.append(remote(gm, gt.at[d, m[d]], GS, 0, p, i, dev(d, i)))
            d1.append(remote(x.at[:, cols[p]], line[p].at[m[d]], D1, 0, p, i, dev(d, i)))
    go(d1)
    xcp = pltpu.make_async_remote_copy(src_ref=x, dst_ref=xs.at[1], send_sem=tsem.at[0], recv_sem=tsem.at[1],
                                       device_id={"tp": 1 - tp}, device_id_type=MESH)
    xcp.start()
    wshared = weights(ws1, ws3, ws2)
    go(wshared)

    def tiles(count, unroll, f):
        def body(q, _):
            for u in range(unroll):
                f(q * unroll + u)
            return 0
        whole = count // unroll
        if whole == 1:
            body(0, 0)
        else:
            lax.fori_loop(0, whole, body, 0)
        for n in range(whole * unroll, count):
            f(n)

    def span(n, w):
        return pl.ds(n * w if isinstance(n, int) else pl.multiple_of(n * w, w), w)

    def up(rows, unroll):
        def f(n):
            ab = jnp.dot(rows(), w13[n], preferred_element_type=F32)
            hid[:, span(n, 128)] = (jax.nn.silu(ab[:, :128]) * ab[:, 128:]).astype(BF)
        tiles(NT, unroll, f)

    def down(store, unroll):
        tiles(8, unroll, lambda n: store(n, jnp.dot(hid[...], w2v[n], preferred_element_type=F32)))

    ri = lax.broadcasted_iota(jnp.int32, (TOK, TOK), 0)
    ra, rb, rs = ri // 64, (ri // 16) % 4, ri % 16
    ex = (mz * 16 + ra * 4 + rb, ra * 16 + rb * 4 + mx, rb * 16 + my * 4 + ra)
    base = tuple(v * CAP + rs for v in ex)

    def picked(c, p, v):
        ps = pt[ORDER[p][0], v] - c * CH
        hit = ps[0:1, :] == base[p]
        for j in range(1, K):
            hit = hit | (ps[j:j + 1, :] == base[p])
        oh = jnp.where(hit, 1.0, 0.0).astype(BF)
        w = jnp.dot(oh, line[p][v], preferred_element_type=F32).astype(BF)
        return w.reshape(4, 4, CH, COLS[p][1])

    def pack(c):
        def body(k, _):
            for p in range(3):
                pk[p][c % 2, k] = picked(c, p, (m[ORDER[p][0]] + k + 1) % 4)
            return 0
        lax.fori_loop(0, 3, body, 0)

    def pack_own():
        def body(c, _):
            for p in range(3):
                po[p][c] = picked(c, p, m[ORDER[p][0]])
            return 0
        lax.fori_loop(0, NC, body, 0)

    def packed(c, p, k):
        return po[p].at[c] if k == 0 else pk[p].at[c % 2, k - 1]

    def s_dst(p, c, b, v):
        return s[p].at[c, :, b, v] if p == 1 else s[p].at[c, :, v, b]

    def d2(c, ks):
        res = []
        for k in ks:
            for i in near:
                for p in range(3):
                    d = ORDER[p][1]
                    res.append(remote(packed(c, p, k).at[at(d, i)], s_dst(p, c, m[d], at(ORDER[p][0], k)),
                                      D2, c, p, i, dev(d, i), k))
        return res

    def d2_own(c, ks):
        res = []
        for k in ks:
            for p in range(3):
                v = m[ORDER[p][1]]
                res.append(local(packed(c, p, k).at[v], s_dst(p, c, v, at(ORDER[p][0], k)), 55 + (c * 3 + p) * 4 + k))
        return res

    def e_at(buf, p, v):
        if p == 0:
            return buf.at[:, :, v, :, cols[0]]
        if p == 1:
            return buf.at[:, v, :, :, cols[1]]
        return buf.at[v, :, :, :, cols[2]]

    def d3(c):
        res = []
        for i in near:
            for p in range(3):
                d = ORDER[p][2]
                res.append(remote(s[p].at[c, at(d, i)], e_at(e.at[c], p, m[d]), D3, c, p, i, dev(d, i)))
        return res

    def load_e(c):
        cps = [local(s[p].at[c, m[ORDER[p][2]]], e_at(ec, p, m[ORDER[p][2]]), 13 + p * 4) for p in range(3)]
        go(cps)
        arrived = d3(c)
        for q, i in enumerate(near):
            for p in range(3):
                arrived[q * 3 + p].wait_recv()
                v = src(ORDER[p][2], i)
                cp = local(e_at(e.at[c], p, v), e_at(ec, p, v), 13 + p * 4 + i)
                cp.start()
                cps.append(cp)
        fin(cps)

    def experts(events):
        def body(b, _):
            for at_b, event in events:
                pl.when(b == at_b)(event)
            z = b % 4
            up(lambda: ec[z].reshape(TOK, D), NT)

            def store(n, v):
                r[(b // 4) % 2, z, :, :, :, span(n, 256)] = v.astype(BF).reshape(4, 4, CH, 256)
            down(store, 8)
            return 0
        lax.fori_loop(0, 4 * NC, body, 0)

    def r3(c):
        res = []
        for i in near:
            for p in range(3):
                d = ORDER[p][2]
                res.append(remote(e_at(r.at[c % 2], p, at(d, i)), q3[p].at[c, m[d]], R3, c, p, i, dev(d, i)))
        return res

    def r3_own(c):
        return [local(e_at(r.at[c % 2], p, m[ORDER[p][2]]), q3[p].at[c, m[ORDER[p][2]]], 25 + c * 3 + p) for p in range(3)]

    def q3_at(p, c, v):
        return q3[p].at[c, :, v] if p == 1 else q3[p].at[c, :, :, v]

    def q2_at(p, c, v):
        return q2[p].at[c, :, v] if p == 2 else q2[p].at[c, v]

    def r2(c):
        res = []
        for i in near:
            for p in range(3):
                d = ORDER[p][1]
                res.append(remote(q3_at(p, c, at(d, i)), q2_at(p, c, m[d]), R2, c, p, i, dev(d, i)))
        return res

    def load_q(c):
        cps = []
        for p in range(3):
            w = m[ORDER[p][1]]
            cps.append(local(q3_at(p, c, w), qv[p].at[w], 34 + p * 4))
        go(cps)
        arrived = r2(c)
        for q, i in enumerate(near):
            for p in range(3):
                arrived[q * 3 + p].wait_recv()
                w = src(ORDER[p][1], i)
                cp = local(q2_at(p, c, w), qv[p].at[w], 34 + p * 4 + i)
                cp.start()
                cps.append(cp)
        fin(cps)

    def add(c, p, i):
        d = ORDER[p][0]
        v = at(d, i)
        ps = pt[d, v] - c * CH
        gs = gt[d, v]
        w = jnp.zeros((TOK, TOK), F32)
        for j in range(K):
            w = w + jnp.where(ps[j:j + 1, :] == base[p], gs[j:j + 1, :], 0.0)
        w1_ = w.astype(BF)
        t = w - w1_.astype(F32)
        w2_ = t.astype(BF)
        w3_ = (t - w2_.astype(F32)).astype(BF)
        rows = qv[p][:, :, v].reshape(TOK, COLS[p][1])
        wt[p, :, 0:TOK] = w1_
        wt[p, :, TOK:2 * TOK] = w2_
        wt[p, :, 2 * TOK:3 * TOK] = w3_
        y = lax.dot_general(wt[p], rows, (((0,), (0,)), ((), ())), preferred_element_type=F32)
        y = (y[2 * TOK:] + y[TOK:2 * TOK]) + y[:TOK]
        acc[i, :, cols[p]] = acc[i, :, cols[p]] + y

    def add_all(c):
        def body(i, _):
            for p in range(3):
                add(c, p, i)
            return 0
        lax.fori_loop(0, 4, body, 0)

    def r1_at(p, i):
        d = ORDER[p][0]
        n = BASE[R1] + p * 3 + i - 1
        return pltpu.make_async_remote_copy(src_ref=acc.at[i, :, cols[p]], dst_ref=fr.at[i, :, cols[p]],
                                            send_sem=ssem.at[n], recv_sem=rsem.at[n],
                                            device_id=dev(d, i), device_id_type=MESH)

    every, rest = (0, 1, 2, 3), (1, 2, 3)
    fin(own_line)
    pack_own()
    for c in range(NC):
        go(d2(c, (0,)))
        go(d2_own(c, (0,)))
    got(d1)
    pack(0)
    go(d2(0, rest))
    go(d2_own(0, rest))

    own_x.wait()
    xcp.wait()
    fin(wshared)

    def shared(k, _):
        up(lambda: xs[k], 4)

        def store(n, v):
            acc[k, :, span(n, 256)] = v
        down(store, 4)
        return 0
    lax.fori_loop(0, 2, shared, 0)
    pcp = pltpu.make_async_remote_copy(src_ref=acc.at[1], dst_ref=prem, send_sem=tsem.at[2], recv_sem=tsem.at[3],
                                       device_id={"tp": 1 - tp}, device_id_type=MESH)
    pcp.start()
    wexp = weights(w1.at[0], w3.at[0], w2.at[0])
    go(wexp)

    pack(1)
    go(d2(1, rest))
    go(d2_own(1, rest))
    got(d2(0, every))
    fin(d2_own(0, every))
    go(d3(0))
    gone(d2(0, rest))
    pack(2)
    go(d2(2, rest))
    go(d2_own(2, rest))
    got(d2(1, every))
    fin(d2_own(1, every))
    go(d3(1))
    pcp.wait()
    acc[0] = acc[0] + (prem[...] + xs[0].astype(F32))
    fin(wexp)

    def first():
        load_e(0)

    def forward():
        got(d2(2, every))
        fin(d2_own(2, every))
        go(d3(2))

    def second():
        go(r3(0))
        go(r3_own(0))
        load_e(1)

    def third():
        go(r3(1))
        go(r3_own(1))
        load_e(2)
        gone(r3(0))
        fin(r3_own(0))

    def middle():
        got(r3(0))
        go(r2(0))
    experts(((0, first), (2, forward), (4, second), (8, third), (10, middle)))
    go(r3(2))
    go(r3_own(2))

    got(r3(1))
    fin(r3_own(1))
    go(r2(1))
    load_q(0)
    acc[1:4] = jnp.zeros((3, TOK, D), F32)
    add_all(0)
    got(r3(2))
    fin(r3_own(2))
    go(r2(2))
    load_q(1)
    add_all(1)
    load_q(2)
    def last(j, _):
        i = (j + 1) % 4
        for p in range(3):
            add(2, p, i)

        @pl.when(j < 3)
        def _():
            for p in range(3):
                r1_at(p, i).start()
        return 0
    lax.fori_loop(0, 4, last, 0)
    res = local(acc.at[0], own, 0)
    res.start()
    fin([r1_at(p, i) for i in range(1, 4) for p in range(3)])
    res.wait()
    gone(d1 + d2(0, (0,)) + d2(1, every) + d2(2, every) + d3(0) + d3(1) + d3(2) + r3(1) + r3(2))
    for c in range(NC):
        gone(r2(c))


def _layer(x, idx, slot, g, ws1, ws3, ws2, w1, w3, w2):
    any_ = pl.BlockSpec(memory_space=pl.ANY)
    vm = pl.BlockSpec(memory_space=pltpu.VMEM)

    def blk(n):
        return jax.ShapeDtypeStruct((NC, 4, 4, 4, CH, n), BF)
    per = [blk(b) for _, b in COLS]
    shapes = [jax.ShapeDtypeStruct((TOK, D), F32)] + per + [blk(D)] + per + per
    shapes += [jax.ShapeDtypeStruct((4, TOK, D), F32)]
    scratch = [pltpu.VMEM((4, TOK, b), BF) for _, b in COLS]
    scratch += [pltpu.VMEM((3, 4, 8, TOK), jnp.int32), pltpu.VMEM((3, 4, 8, TOK), F32)]
    scratch += [pltpu.VMEM((8, TOK), jnp.int32), pltpu.VMEM((8, TOK), F32)]
    scratch += [pltpu.VMEM((3, TOK, 3 * TOK), BF)]
    scratch += [pltpu.VMEM((2, 3, 4, 4, CH, b), BF) for _, b in COLS]
    scratch += [pltpu.VMEM((NC, 4, 4, CH, b), BF) for _, b in COLS]
    scratch += [pltpu.VMEM((4, 4, 4, CH, D), BF)]
    scratch += [pltpu.VMEM((4, 4, 4, CH, b), BF) for _, b in COLS]
    scratch += [
        pltpu.VMEM((2, 4, 4, 4, CH, D), BF),
        pltpu.VMEM((NT, D, 256), BF),
        pltpu.VMEM((8, F, 256), BF),
        pltpu.VMEM((TOK, F), BF),
        pltpu.VMEM((4, TOK, D), F32),
        pltpu.VMEM((2, TOK, D), BF),
        pltpu.VMEM((TOK, D), F32),
        pltpu.SemaphoreType.DMA((NSEM,)),
        pltpu.SemaphoreType.DMA((NSEM,)),
        pltpu.SemaphoreType.DMA((91,)),
        pltpu.SemaphoreType.DMA((2 * NT + 8,)),
        pltpu.SemaphoreType.DMA((4,)),
    ]
    res = pl.pallas_call(
        _kernel,
        out_shape=shapes,
        in_specs=[any_, vm, vm, vm] + [any_] * 6,
        out_specs=[any_] * len(shapes),
        scratch_shapes=scratch,
        compiler_params=pltpu.CompilerParams(collective_id=0, has_side_effects=True, vmem_limit_bytes=67043328),
    )(x, idx, slot, g, ws1, ws3, ws2, w1, w3, w2)
    own, others = res[0], res[-1]
    return ((own + others[1]) + (others[2] + others[3])).astype(BF)


def solution(mesh):
    rows = P(("ep", "tp"), None)

    def body(x, idx, g, slot, ws1, ws3, ws2, w1, w3, w2):
        return _layer(x, idx.T, slot.T, g.T, ws1, ws3, ws2, w1, w3, w2)

    return jax.shard_map(
        body, mesh=mesh,
        in_specs=(rows, rows, rows, rows, P(None, "tp"), P(None, "tp"), P("tp", None),
                  P("ep", None, None), P("ep", None, None), P("ep", None, None)),
        out_specs=rows, check_vma=False)
```

```python
import jax
import jax.numpy as jnp
from jax import lax
from jax.experimental import pallas as pl
from jax.experimental.pallas import tpu as pltpu
from jax.sharding import PartitionSpec as P

MESH = pl.DeviceIdType.MESH
BF = jnp.bfloat16
F32 = jnp.float32

TOK = 256
D = 2048
F = 1408
K = 6
CAP = 48
CH = 16
NC = CAP // CH
NT = F // 128

COLS = ((0, 640), (640, 640), (1280, 768))
ORDER = ((0, 1, 2), (2, 0, 1), (1, 2, 0))
D1, PS, GS, R1, D2, D3, R3, R2 = range(8)
BASE = {D1: 0, PS: 9, GS: 18, D3: 27, R3: 54, R2: 81, D2: 108, R1: 216}
NSEM = 216 + 18


def _sem(stage, c, p, i, k):
    if stage == D2:
        return BASE[D2] + ((c * 3 + p) * 3 + i - 1) * 4 + k
    return BASE[stage] + (c * 3 + p) * 3 + i - 1


def _kernel(x, idx, slot, g, ws1, ws3, ws2, w1, w3, w2,
            own, sa, sb, sc, e, q3a, q3b, q3c, q2a, q2b, q2c, fr,
            la, lb, lc, pt, gt, pm, gm, wt, pa, pb, pc, oa, ob, oc, ec, qa, qb, qc, r, w13, w2v, hid,
            acc, mid, xs, prem, ssem, rsem, lsem, wsem, tsem):
    ep = lax.axis_index("ep")
    tp = lax.axis_index("tp")
    z0, y0, x0 = ep // 16, lax.rem(ep // 4, 4), lax.rem(ep, 4)
    m = (z0 + tp * (y0 - z0), y0 + tp * (x0 - y0), x0 + tp * (z0 - x0))
    mz, my, mx = m
    kz, ky, kx = 16 - 12 * tp, 4 - 3 * tp, 1 + 15 * tp
    s = (sa, sb, sc)
    q3 = (q3a, q3b, q3c)
    q2 = (q2a, q2b, q2c)
    line = (la, lb, lc)
    pk = (pa, pb, pc)
    po = (oa, ob, oc)
    qv = (qa, qb, qc)
    cols = tuple(pl.ds(a, b) for a, b in COLS)

    AT = [[m[d] if i == 0 else lax.rem(m[d] + i, 4) for i in range(4)] for d in range(3)]
    DEV = [[kz * (AT[0][i] if d == 0 else mz) + ky * (AT[1][i] if d == 1 else my) + kx * (AT[2][i] if d == 2 else mx)
            for i in range(4)] for d in range(3)]

    def dev(d, i):
        return {"ep": DEV[d][i]}

    def at(d, i):
        return AT[d][i] if isinstance(i, int) else lax.rem(m[d] + i, 4)

    def src(d, i):
        return AT[d][(4 - i) % 4]

    def weights(u1, u3, u2):
        cps = []
        for n in range(NT):
            cps.append(pltpu.make_async_copy(u1.at[:, pl.ds(n * 128, 128)], w13.at[n, :, pl.ds(0, 128)], wsem.at[2 * n]))
            cps.append(pltpu.make_async_copy(u3.at[:, pl.ds(n * 128, 128)], w13.at[n, :, pl.ds(128, 128)], wsem.at[2 * n + 1]))
        for n in range(8):
            cps.append(pltpu.make_async_copy(u2.at[:, pl.ds(n * 256, 256)], w2v.at[n], wsem.at[2 * NT + n]))
        return cps

    bar = pltpu.get_barrier_semaphore()
    for d in range(3):
        for i in range(1, 4):
            pl.semaphore_signal(bar, inc=1, device_id=dev(d, i), device_id_type=MESH)
    pl.semaphore_signal(bar, inc=1, device_id={"tp": 1 - tp}, device_id_type=MESH)

    own_x = pltpu.make_async_copy(x, xs.at[0], lsem.at[0])
    own_x.start()
    own_line = [pltpu.make_async_copy(x.at[:, cols[p]], line[p].at[m[ORDER[p][0]]], lsem.at[1 + p]) for p in range(3)]
    for c in own_line:
        c.start()
    pm[...] = jnp.full((8, TOK), -1, jnp.int32)
    gm[...] = jnp.zeros((8, TOK), F32)
    pm[0:K, :] = jnp.where(slot[...] >= 0, idx[...] * CAP + slot[...], -1)
    gm[0:K, :] = g[...]
    for d in range(3):
        pt[d, m[d]] = pm[...]
        gt[d, m[d]] = gm[...]
    pl.semaphore_wait(bar, 10)

    def remote(a, b, stage, c, p, i, where, k=0):
        n = _sem(stage, c, p, i, k)
        return pltpu.make_async_remote_copy(src_ref=a, dst_ref=b, send_sem=ssem.at[n], recv_sem=rsem.at[n],
                                            device_id=where, device_id_type=MESH)

    def local(a, b, n):
        return pltpu.make_async_copy(a, b, lsem.at[n])

    def go(cps):
        for cp in cps:
            cp.start()

    def fin(cps):
        for cp in cps:
            cp.wait()

    def got(cps):
        for cp in cps:
            cp.wait_recv()

    def gone(cps):
        for cp in cps:
            cp.wait_send()

    near = (1, 3, 2)

    d1 = []
    for i in near:
        for p in range(3):
            d = ORDER[p][0]
            d1.append(remote(pm, pt.at[d, m[d]], PS, 0, p, i, dev(d, i)))
            d1.append(remote(gm, gt.at[d, m[d]], GS, 0, p, i, dev(d, i)))
            d1.append(remote(x.at[:, cols[p]], line[p].at[m[d]], D1, 0, p, i, dev(d, i)))
    go(d1)
    xcp = pltpu.make_async_remote_copy(src_ref=x, dst_ref=xs.at[1], send_sem=tsem.at[0], recv_sem=tsem.at[1],
                                       device_id={"tp": 1 - tp}, device_id_type=MESH)
    xcp.start()
    wshared = weights(ws1, ws3, ws2)
    go(wshared)

    def tiles(count, unroll, f):
        def body(q, _):
            for u in range(unroll):
                f(q * unroll + u)
            return 0
        whole = count // unroll
        if whole == 1:
            body(0, 0)
        else:
            lax.fori_loop(0, whole, body, 0)
        for n in range(whole * unroll, count):
            f(n)

    def span(n, w):
        return pl.ds(n * w if isinstance(n, int) else pl.multiple_of(n * w, w), w)

    def up(rows, unroll):
        def f(n):
            ab = jnp.dot(rows(), w13[n], preferred_element_type=F32)
            hid[:, span(n, 128)] = (jax.nn.silu(ab[:, :128]) * ab[:, 128:]).astype(BF)
        tiles(NT, unroll, f)

    def down(store, unroll):
        tiles(8, unroll, lambda n: store(n, jnp.dot(hid[...], w2v[n], preferred_element_type=F32)))

    ri = lax.broadcasted_iota(jnp.int32, (TOK, TOK), 0)
    ra, rb, rs = ri // 64, (ri // 16) % 4, ri % 16
    ex = (mz * kz + ra * ky + rb * kx, ra * kz + rb * ky + mx * kx, rb * kz + my * ky + ra * kx)
    base = tuple(v * CAP + rs for v in ex)

    def picked(c, p, v):
        ps = pt[ORDER[p][0], v] - c * CH
        hit = ps[0:1, :] == base[p]
        for j in range(1, K):
            hit = hit | (ps[j:j + 1, :] == base[p])
        oh = jnp.where(hit, 1.0, 0.0).astype(BF)
        w = jnp.dot(oh, line[p][v], preferred_element_type=F32).astype(BF)
        return w.reshape(4, 4, CH, COLS[p][1])

    def pack(c):
        def body(k, _):
            for p in range(3):
                pk[p][c % 2 if isinstance(c, int) else lax.rem(c, 2), k] = picked(c, p, at(ORDER[p][0], k + 1))
            return 0
        lax.fori_loop(0, 3, body, 0)

    def pack_own():
        def body(c, _):
            for p in range(3):
                po[p][c] = picked(c, p, m[ORDER[p][0]])
            return 0
        lax.fori_loop(0, NC, body, 0)

    def packed(c, p, k):
        return po[p].at[c] if k == 0 else pk[p].at[c % 2, k - 1]

    def s_dst(p, c, b, v):
        return s[p].at[c, :, b, v] if p == 1 else s[p].at[c, :, v, b]

    def d2(c, ks):
        res = []
        for k in ks:
            for i in near:
                for p in range(3):
                    d = ORDER[p][1]
                    res.append(remote(packed(c, p, k).at[at(d, i)], s_dst(p, c, m[d], at(ORDER[p][0], k)),
                                      D2, c, p, i, dev(d, i), k))
        return res

    def d2_own(c, ks):
        res = []
        for k in ks:
            for p in range(3):
                v = m[ORDER[p][1]]
                res.append(local(packed(c, p, k).at[v], s_dst(p, c, v, at(ORDER[p][0], k)), 55 + (c * 3 + p) * 4 + k))
        return res

    def e_at(buf, p, v):
        if p == 0:
            return buf.at[:, :, v, :, cols[0]]
        if p == 1:
            return buf.at[:, v, :, :, cols[1]]
        return buf.at[v, :, :, :, cols[2]]

    def d3(c):
        res = []
        for i in near:
            for p in range(3):
                d = ORDER[p][2]
                res.append(remote(s[p].at[c, at(d, i)], e_at(e.at[c], p, m[d]), D3, c, p, i, dev(d, i)))
        return res

    def load_e(c):
        cps = [local(s[p].at[c, m[ORDER[p][2]]], e_at(ec, p, m[ORDER[p][2]]), 13 + p * 4) for p in range(3)]
        go(cps)
        arrived = d3(c)
        for q, i in enumerate(near):
            for p in range(3):
                arrived[q * 3 + p].wait_recv()
                v = src(ORDER[p][2], i)
                cp = local(e_at(e.at[c], p, v), e_at(ec, p, v), 13 + p * 4 + i)
                cp.start()
                cps.append(cp)
        fin(cps)

    def experts(events):
        def body(b, _):
            for at_b, event in events:
                pl.when(b == at_b)(event)
            z = lax.rem(b, 4)
            up(lambda: ec[z].reshape(TOK, D), NT)

            def store(n, v):
                r[lax.rem(b // 4, 2), z, :, :, :, span(n, 256)] = v.astype(BF).reshape(4, 4, CH, 256)
            down(store, 8)
            return 0
        lax.fori_loop(0, 4 * NC, body, 0)

    def r3(c):
        res = []
        for i in near:
            for p in range(3):
                d = ORDER[p][2]
                res.append(remote(e_at(r.at[c % 2], p, at(d, i)), q3[p].at[c, m[d]], R3, c, p, i, dev(d, i)))
        return res

    def r3_own(c):
        return [local(e_at(r.at[c % 2], p, m[ORDER[p][2]]), q3[p].at[c, m[ORDER[p][2]]], 25 + c * 3 + p) for p in range(3)]

    def q3_at(p, c, v):
        return q3[p].at[c, :, v] if p == 1 else q3[p].at[c, :, :, v]

    def q2_at(p, c, v):
        return q2[p].at[c, :, v] if p == 2 else q2[p].at[c, v]

    def r2(c):
        res = []
        for i in near:
            for p in range(3):
                d = ORDER[p][1]
                res.append(remote(q3_at(p, c, at(d, i)), q2_at(p, c, m[d]), R2, c, p, i, dev(d, i)))
        return res

    def load_q(c):
        cps = []
        for p in range(3):
            w = m[ORDER[p][1]]
            cps.append(local(q3_at(p, c, w), qv[p].at[w], 34 + p * 4))
        go(cps)
        arrived = r2(c)
        for q, i in enumerate(near):
            for p in range(3):
                arrived[q * 3 + p].wait_recv()
                w = src(ORDER[p][1], i)
                cp = local(q2_at(p, c, w), qv[p].at[w], 34 + p * 4 + i)
                cp.start()
                cps.append(cp)
        fin(cps)

    def add(c, p, i):
        d = ORDER[p][0]
        v = at(d, i)
        ps = pt[d, v] - c * CH
        gs = gt[d, v]
        w = jnp.zeros((TOK, TOK), F32)
        for j in range(K):
            w = w + jnp.where(ps[j:j + 1, :] == base[p], gs[j:j + 1, :], 0.0)
        w1_ = w.astype(BF)
        t = w - w1_.astype(F32)
        w2_ = t.astype(BF)
        w3_ = (t - w2_.astype(F32)).astype(BF)
        rows = qv[p][:, :, v].reshape(TOK, COLS[p][1])
        wt[p, :, 0:TOK] = w1_
        wt[p, :, TOK:2 * TOK] = w2_
        wt[p, :, 2 * TOK:3 * TOK] = w3_
        y = lax.dot_general(wt[p], rows, (((0,), (0,)), ((), ())), preferred_element_type=F32)
        y = (y[2 * TOK:] + y[TOK:2 * TOK]) + y[:TOK]
        acc[i, :, cols[p]] = acc[i, :, cols[p]] + y

    def add_all(c):
        def body(i, _):
            for p in range(3):
                add(c, p, i)
            return 0
        lax.fori_loop(0, 4, body, 0)

    half = (pl.ds(0, TOK // 2), pl.ds(TOK // 2, TOK // 2))

    def r1(q):
        res = []
        for p in range(3):
            d = ORDER[p][0]
            n = BASE[R1] + p * 6 + q
            up_ = q % 2 == 0
            if q < 2:
                a, b = acc.at[2, half[q], cols[p]], mid.at[q, :, cols[p]]
            else:
                rows = half[{2: 1, 3: 0, 4: 0, 5: 1}[q]]
                a, b = acc.at[1 if up_ else 3, rows, cols[p]], fr.at[0 if up_ else 1, rows, cols[p]]
            res.append(pltpu.make_async_remote_copy(src_ref=a, dst_ref=b, send_sem=ssem.at[n], recv_sem=rsem.at[n],
                                                    device_id=dev(d, 1 if up_ else 3), device_id_type=MESH))
        return res

    every, rest = (0, 1, 2, 3), (1, 2, 3)
    fin(own_line)
    pack_own()
    for c in range(NC):
        go(d2(c, (0,)))
        go(d2_own(c, (0,)))
    got(d1)
    pack(0)
    go(d2(0, rest))
    go(d2_own(0, rest))

    own_x.wait()
    xcp.wait()
    fin(wshared)

    def shared(k, _):
        up(lambda: xs[k], 4)

        def store(n, v):
            acc[k, :, span(n, 256)] = v
        down(store, 4)
        return 0
    lax.fori_loop(0, 2, shared, 0)
    pcp = pltpu.make_async_remote_copy(src_ref=acc.at[1], dst_ref=prem, send_sem=tsem.at[2], recv_sem=tsem.at[3],
                                       device_id={"tp": 1 - tp}, device_id_type=MESH)
    pcp.start()
    wexp = weights(w1.at[0], w3.at[0], w2.at[0])
    go(wexp)

    pack(1)
    go(d2(1, rest))
    go(d2_own(1, rest))
    got(d2(0, every))
    fin(d2_own(0, every))
    go(d3(0))
    gone(d2(0, rest))
    pack(2)
    go(d2(2, rest))
    go(d2_own(2, rest))
    got(d2(1, every))
    fin(d2_own(1, every))
    go(d3(1))
    pcp.wait()
    acc[0] = acc[0] + (prem[...] + xs[0].astype(F32))
    fin(wexp)

    def first():
        load_e(0)

    def forward():
        got(d2(2, every))
        fin(d2_own(2, every))
        go(d3(2))

    def second():
        go(r3(0))
        go(r3_own(0))
        load_e(1)

    def third():
        go(r3(1))
        go(r3_own(1))
        load_e(2)
        gone(r3(0))
        fin(r3_own(0))

    def middle():
        got(r3(0))
        go(r2(0))
    experts(((0, first), (2, forward), (4, second), (8, third), (10, middle)))
    go(r3(2))
    go(r3_own(2))

    got(r3(1))
    fin(r3_own(1))
    go(r2(1))
    load_q(0)
    acc[1:4] = jnp.zeros((3, TOK, D), F32)
    add_all(0)
    got(r3(2))
    fin(r3_own(2))
    go(r2(2))
    load_q(1)
    add_all(1)
    load_q(2)
    def last(j, _):
        i = lax.rem(2 + 3 * j, 4)
        for p in range(3):
            add(2, p, i)

        @pl.when(j == 0)
        def _():
            go(r1(0))
            go(r1(1))

        @pl.when(j == 1)
        def _():
            go(r1(2))
        return 0
    lax.fori_loop(0, 4, last, 0)
    go(r1(3))
    res = local(acc.at[0], own, 0)
    res.start()
    for q in range(2):
        i = 1 + 2 * q
        via, on = r1(q), r1(4 + q)
        for p in range(3):
            via[p].wait_recv()
            acc[i, half[q], cols[p]] = acc[i, half[q], cols[p]] + mid[q, :, cols[p]]
            on[p].start()
    for q in range(2):
        gone(r1(q))
        fin(r1(2 + q))
        fin(r1(4 + q))
    res.wait()
    gone(d1 + d2(0, (0,)) + d2(1, every) + d2(2, every) + d3(0) + d3(1) + d3(2) + r3(1) + r3(2))
    for c in range(NC):
        gone(r2(c))


def _layer(x, idx, slot, g, ws1, ws3, ws2, w1, w3, w2):
    any_ = pl.BlockSpec(memory_space=pl.ANY)
    vm = pl.BlockSpec(memory_space=pltpu.VMEM)

    def blk(n):
        return jax.ShapeDtypeStruct((NC, 4, 4, 4, CH, n), BF)
    per = [blk(b) for _, b in COLS]
    shapes = [jax.ShapeDtypeStruct((TOK, D), F32)] + per + [blk(D)] + per + per
    shapes += [jax.ShapeDtypeStruct((2, TOK, D), F32)]
    scratch = [pltpu.VMEM((4, TOK, b), BF) for _, b in COLS]
    scratch += [pltpu.VMEM((3, 4, 8, TOK), jnp.int32), pltpu.VMEM((3, 4, 8, TOK), F32)]
    scratch += [pltpu.VMEM((8, TOK), jnp.int32), pltpu.VMEM((8, TOK), F32)]
    scratch += [pltpu.VMEM((3, TOK, 3 * TOK), BF)]
    scratch += [pltpu.VMEM((2, 3, 4, 4, CH, b), BF) for _, b in COLS]
    scratch += [pltpu.VMEM((NC, 4, 4, CH, b), BF) for _, b in COLS]
    scratch += [pltpu.VMEM((4, 4, 4, CH, D), BF)]
    scratch += [pltpu.VMEM((4, 4, 4, CH, b), BF) for _, b in COLS]
    scratch += [
        pltpu.VMEM((2, 4, 4, 4, CH, D), BF),
        pltpu.VMEM((NT, D, 256), BF),
        pltpu.VMEM((8, F, 256), BF),
        pltpu.VMEM((TOK, F), BF),
        pltpu.VMEM((4, TOK, D), F32),
        pltpu.VMEM((2, TOK // 2, D), F32),
        pltpu.VMEM((2, TOK, D), BF),
        pltpu.VMEM((TOK, D), F32),
        pltpu.SemaphoreType.DMA((NSEM,)),
        pltpu.SemaphoreType.DMA((NSEM,)),
        pltpu.SemaphoreType.DMA((91,)),
        pltpu.SemaphoreType.DMA((2 * NT + 8,)),
        pltpu.SemaphoreType.DMA((4,)),
    ]
    res = pl.pallas_call(
        _kernel,
        out_shape=shapes,
        in_specs=[any_, vm, vm, vm] + [any_] * 6,
        out_specs=[any_] * len(shapes),
        scratch_shapes=scratch,
        compiler_params=pltpu.CompilerParams(collective_id=0, has_side_effects=True, vmem_limit_bytes=67043328),
    )(x, idx, slot, g, ws1, ws3, ws2, w1, w3, w2)
    own, others = res[0], res[-1]
    return (own + (others[0] + others[1])).astype(BF)


def solution(mesh):
    rows = P(("ep", "tp"), None)

    def body(x, idx, g, slot, ws1, ws3, ws2, w1, w3, w2):
        return _layer(x, idx.T, slot.T, g.T, ws1, ws3, ws2, w1, w3, w2)

    return jax.shard_map(
        body, mesh=mesh,
        in_specs=(rows, rows, rows, rows, P(None, "tp"), P(None, "tp"), P("tp", None),
                  P("ep", None, None), P("ep", None, None), P("ep", None, None)),
        out_specs=rows, check_vma=False)
```

```python
import jax
import jax.numpy as jnp
from jax import lax
from jax.experimental import pallas as pl
from jax.experimental.pallas import tpu as pltpu
from jax.sharding import PartitionSpec as P

MESH = pl.DeviceIdType.MESH
BF = jnp.bfloat16
F32 = jnp.float32

TOK = 256
D = 2048
F = 1408
K = 6
CAP = 48
CH = 16
NC = CAP // CH
NT = F // 128

COLS = ((0, 640), (640, 640), (1280, 768))
ORDER = ((0, 1, 2), (2, 0, 1), (1, 2, 0))
D1, PS, GS, R1, D2, D3, R3, R2 = range(8)
BASE = {D1: 0, PS: 9, GS: 18, D3: 27, R3: 54, R2: 81, D2: 108, R1: 216}
NSEM = 216 + 18 + 3


def _sem(stage, c, p, i, k):
    if stage == D2:
        return BASE[D2] + ((c * 3 + p) * 3 + i - 1) * 4 + k
    return BASE[stage] + (c * 3 + p) * 3 + i - 1


def _kernel(x, idx, slot, g, ws1, ws3, ws2, w1, w3, w2,
            own, sa, sb, sc, e, q3a, q3b, q3c, q2a, q2b, q2c, fr,
            la, lb, lc, iv, sv, gv, pt, gt, pm, gm, wt, pa, pb, pc, oa, ob, oc, ec, qa, qb, qc, r, w13, w2v, hid,
            acc, mid, xs, prem, ssem, rsem, lsem, wsem, tsem):
    ep = lax.axis_index("ep")
    tp = lax.axis_index("tp")
    z0, y0, x0 = ep // 16, lax.rem(ep // 4, 4), lax.rem(ep, 4)
    m = (z0 + tp * (y0 - z0), y0 + tp * (x0 - y0), x0 + tp * (z0 - x0))
    mz, my, mx = m
    kz, ky, kx = 16 - 12 * tp, 4 - 3 * tp, 1 + 15 * tp
    s = (sa, sb, sc)
    q3 = (q3a, q3b, q3c)
    q2 = (q2a, q2b, q2c)
    line = (la, lb, lc)
    pk = (pa, pb, pc)
    po = (oa, ob, oc)
    qv = (qa, qb, qc)
    cols = tuple(pl.ds(a, b) for a, b in COLS)

    AT = [[m[d] if i == 0 else lax.rem(m[d] + i, 4) for i in range(4)] for d in range(3)]
    DEV = [[kz * (AT[0][i] if d == 0 else mz) + ky * (AT[1][i] if d == 1 else my) + kx * (AT[2][i] if d == 2 else mx)
            for i in range(4)] for d in range(3)]

    def dev(d, i):
        return {"ep": DEV[d][i]}

    def at(d, i):
        return AT[d][i] if isinstance(i, int) else lax.rem(m[d] + i, 4)

    def src(d, i):
        return AT[d][(4 - i) % 4]

    def weights(u1, u3, u2):
        cps = []
        for n in range(NT):
            cps.append(pltpu.make_async_copy(u1.at[:, pl.ds(n * 128, 128)], w13.at[n, :, pl.ds(0, 128)], wsem.at[2 * n]))
            cps.append(pltpu.make_async_copy(u3.at[:, pl.ds(n * 128, 128)], w13.at[n, :, pl.ds(128, 128)], wsem.at[2 * n + 1]))
        for n in range(8):
            cps.append(pltpu.make_async_copy(u2.at[:, pl.ds(n * 256, 256)], w2v.at[n], wsem.at[2 * NT + n]))
        return cps

    small = [pltpu.make_async_copy(a, b, lsem.at[91 + n]) for n, (a, b) in enumerate(((idx, iv), (slot, sv), (g, gv)))]
    for c in small:
        c.start()

    bar = pltpu.get_barrier_semaphore()
    for d in range(3):
        for i in range(1, 4):
            pl.semaphore_signal(bar, inc=1, device_id=dev(d, i), device_id_type=MESH)
    pl.semaphore_signal(bar, inc=1, device_id={"tp": 1 - tp}, device_id_type=MESH)

    own_x = pltpu.make_async_copy(x, xs.at[0], lsem.at[0])
    own_x.start()
    own_line = [pltpu.make_async_copy(x.at[:, cols[p]], line[p].at[m[ORDER[p][0]]], lsem.at[1 + p]) for p in range(3)]
    for c in own_line:
        c.start()
    pm[...] = jnp.full((8, TOK), -1, jnp.int32)
    gm[...] = jnp.zeros((8, TOK), F32)
    for c in small:
        c.wait()
    pm[0:K, :] = jnp.where(sv[...] >= 0, iv[...] * CAP + sv[...], -1)
    gm[0:K, :] = gv[...]
    for d in range(3):
        pt[d, m[d]] = pm[...]
        gt[d, m[d]] = gm[...]
    pl.semaphore_wait(bar, 10)

    def remote(a, b, stage, c, p, i, where, k=0):
        n = _sem(stage, c, p, i, k)
        return pltpu.make_async_remote_copy(src_ref=a, dst_ref=b, send_sem=ssem.at[n], recv_sem=rsem.at[n],
                                            device_id=where, device_id_type=MESH)

    def local(a, b, n):
        return pltpu.make_async_copy(a, b, lsem.at[n])

    def go(cps):
        for cp in cps:
            cp.start()

    def fin(cps):
        for cp in cps:
            cp.wait()

    def got(cps):
        for cp in cps:
            cp.wait_recv()

    def gone(cps):
        for cp in cps:
            cp.wait_send()

    near = (1, 3, 2)

    half = (pl.ds(0, TOK // 2), pl.ds(TOK // 2, TOK // 2))
    d1 = []
    for i in (1, 3):
        for p in range(3):
            d = ORDER[p][0]
            d1.append(remote(x.at[:, cols[p]], line[p].at[m[d]], D1, 0, p, i, dev(d, i)))
    d1s = []
    for i in near:
        for p in range(3):
            d = ORDER[p][0]
            d1s.append(remote(pm, pt.at[d, m[d]], PS, 0, p, i, dev(d, i)))
            d1s.append(remote(gm, gt.at[d, m[d]], GS, 0, p, i, dev(d, i)))

    def passed(q):
        res = []
        for p in range(3):
            d = ORDER[p][0]
            v = line[p].at[AT[d][3 - 2 * q], half[q]]
            n = BASE[D1] + p * 3 + 1 if q == 0 else 234 + p
            res.append(pltpu.make_async_remote_copy(src_ref=v, dst_ref=v, send_sem=ssem.at[n], recv_sem=rsem.at[n],
                                                    device_id=dev(d, 1 + 2 * q), device_id_type=MESH))
        return res
    go(d1)
    go(d1s)
    xcp = pltpu.make_async_remote_copy(src_ref=x, dst_ref=xs.at[1], send_sem=tsem.at[0], recv_sem=tsem.at[1],
                                       device_id={"tp": 1 - tp}, device_id_type=MESH)
    xcp.start()
    wshared = weights(ws1, ws3, ws2)
    go(wshared)

    def tiles(count, unroll, f):
        def body(q, _):
            for u in range(unroll):
                f(q * unroll + u)
            return 0
        whole = count // unroll
        if whole == 1:
            body(0, 0)
        else:
            lax.fori_loop(0, whole, body, 0)
        for n in range(whole * unroll, count):
            f(n)

    def span(n, w):
        return pl.ds(n * w if isinstance(n, int) else pl.multiple_of(n * w, w), w)

    def up(rows, unroll):
        def f(n):
            ab = jnp.dot(rows(), w13[n], preferred_element_type=F32)
            hid[:, span(n, 128)] = (jax.nn.silu(ab[:, :128]) * ab[:, 128:]).astype(BF)
        tiles(NT, unroll, f)

    def down(store, unroll):
        tiles(8, unroll, lambda n: store(n, jnp.dot(hid[...], w2v[n], preferred_element_type=F32)))

    ri = lax.broadcasted_iota(jnp.int32, (TOK, TOK), 0)
    ra, rb, rs = ri // 64, (ri // 16) % 4, ri % 16
    ex = (mz * kz + ra * ky + rb * kx, ra * kz + rb * ky + mx * kx, rb * kz + my * ky + ra * kx)
    base = tuple(v * CAP + rs for v in ex)

    def picked(c, p, v):
        ps = pt[ORDER[p][0], v] - c * CH
        hit = ps[0:1, :] == base[p]
        for j in range(1, K):
            hit = hit | (ps[j:j + 1, :] == base[p])
        oh = jnp.where(hit, 1.0, 0.0).astype(BF)
        w = jnp.dot(oh, line[p][v], preferred_element_type=F32).astype(BF)
        return w.reshape(4, 4, CH, COLS[p][1])

    def pack(c):
        def body(k, _):
            for p in range(3):
                pk[p][c % 2 if isinstance(c, int) else lax.rem(c, 2), k] = picked(c, p, at(ORDER[p][0], k + 1))
            return 0
        lax.fori_loop(0, 3, body, 0)

    def pack_own():
        def body(c, _):
            for p in range(3):
                po[p][c] = picked(c, p, m[ORDER[p][0]])
            return 0
        lax.fori_loop(0, NC, body, 0)

    def packed(c, p, k):
        return po[p].at[c] if k == 0 else pk[p].at[c % 2, k - 1]

    def s_dst(p, c, b, v):
        return s[p].at[c, :, b, v] if p == 1 else s[p].at[c, :, v, b]

    def d2(c, ks):
        res = []
        for k in ks:
            for i in near:
                for p in range(3):
                    d = ORDER[p][1]
                    res.append(remote(packed(c, p, k).at[at(d, i)], s_dst(p, c, m[d], at(ORDER[p][0], k)),
                                      D2, c, p, i, dev(d, i), k))
        return res

    def d2_own(c, ks):
        res = []
        for k in ks:
            for p in range(3):
                v = m[ORDER[p][1]]
                res.append(local(packed(c, p, k).at[v], s_dst(p, c, v, at(ORDER[p][0], k)), 55 + (c * 3 + p) * 4 + k))
        return res

    def e_at(buf, p, v):
        if p == 0:
            return buf.at[:, :, v, :, cols[0]]
        if p == 1:
            return buf.at[:, v, :, :, cols[1]]
        return buf.at[v, :, :, :, cols[2]]

    def d3(c):
        res = []
        for i in near:
            for p in range(3):
                d = ORDER[p][2]
                res.append(remote(s[p].at[c, at(d, i)], e_at(e.at[c], p, m[d]), D3, c, p, i, dev(d, i)))
        return res

    def load_e(c):
        cps = [local(s[p].at[c, m[ORDER[p][2]]], e_at(ec, p, m[ORDER[p][2]]), 13 + p * 4) for p in range(3)]
        go(cps)
        arrived = d3(c)
        for q, i in enumerate(near):
            for p in range(3):
                arrived[q * 3 + p].wait_recv()
                v = src(ORDER[p][2], i)
                cp = local(e_at(e.at[c], p, v), e_at(ec, p, v), 13 + p * 4 + i)
                cp.start()
                cps.append(cp)
        fin(cps)

    def experts(events):
        def body(b, _):
            for at_b, event in events:
                pl.when(b == at_b)(event)
            z = lax.rem(b, 4)
            up(lambda: ec[z].reshape(TOK, D), NT)

            def store(n, v):
                r[lax.rem(b // 4, 2), z, :, :, :, span(n, 256)] = v.astype(BF).reshape(4, 4, CH, 256)
            down(store, 8)
            return 0
        lax.fori_loop(0, 4 * NC, body, 0)

    def r3(c):
        res = []
        for i in near:
            for p in range(3):
                d = ORDER[p][2]
                res.append(remote(e_at(r.at[c % 2], p, at(d, i)), q3[p].at[c, m[d]], R3, c, p, i, dev(d, i)))
        return res

    def r3_own(c):
        return [local(e_at(r.at[c % 2], p, m[ORDER[p][2]]), q3[p].at[c, m[ORDER[p][2]]], 25 + c * 3 + p) for p in range(3)]

    def q3_at(p, c, v):
        return q3[p].at[c, :, v] if p == 1 else q3[p].at[c, :, :, v]

    def q2_at(p, c, v):
        return q2[p].at[c, :, v] if p == 2 else q2[p].at[c, v]

    def r2(c):
        res = []
        for i in near:
            for p in range(3):
                d = ORDER[p][1]
                res.append(remote(q3_at(p, c, at(d, i)), q2_at(p, c, m[d]), R2, c, p, i, dev(d, i)))
        return res

    def load_q(c):
        cps = []
        for p in range(3):
            w = m[ORDER[p][1]]
            cps.append(local(q3_at(p, c, w), qv[p].at[w], 34 + p * 4))
        go(cps)
        arrived = r2(c)
        for q, i in enumerate(near):
            for p in range(3):
                arrived[q * 3 + p].wait_recv()
                w = src(ORDER[p][1], i)
                cp = local(q2_at(p, c, w), qv[p].at[w], 34 + p * 4 + i)
                cp.start()
                cps.append(cp)
        fin(cps)

    def weigh(c, p, i):
        d = ORDER[p][0]
        v = at(d, i)
        ps = pt[d, v] - c * CH
        gs = gt[d, v]
        w = jnp.zeros((TOK, TOK), F32)
        for j in range(K):
            w = w + jnp.where(ps[j:j + 1, :] == base[p], gs[j:j + 1, :], 0.0)
        w1_ = w.astype(BF)
        t = w - w1_.astype(F32)
        w2_ = t.astype(BF)
        w3_ = (t - w2_.astype(F32)).astype(BF)
        wt[p, :, 0:TOK] = w1_
        wt[p, :, TOK:2 * TOK] = w2_
        wt[p, :, 2 * TOK:3 * TOK] = w3_

    def add(p, i):
        rows = qv[p][:, :, at(ORDER[p][0], i)].reshape(TOK, COLS[p][1])
        y = lax.dot_general(wt[p], rows, (((0,), (0,)), ((), ())), preferred_element_type=F32)
        y = (y[2 * TOK:] + y[TOK:2 * TOK]) + y[:TOK]
        acc[i, :, cols[p]] = acc[i, :, cols[p]] + y

    def add_all(c):
        def body(i, _):
            for p in range(3):
                weigh(c, p, i)
                add(p, i)
            return 0
        lax.fori_loop(0, 4, body, 0)

    def r1(q):
        res = []
        for p in range(3):
            d = ORDER[p][0]
            n = BASE[R1] + p * 6 + q
            up_ = q % 2 == 0
            if q < 2:
                a, b = acc.at[2, half[q], cols[p]], mid.at[q, :, cols[p]]
            else:
                rows = half[{2: 1, 3: 0, 4: 0, 5: 1}[q]]
                a, b = acc.at[1 if up_ else 3, rows, cols[p]], fr.at[0 if up_ else 1, rows, cols[p]]
            res.append(pltpu.make_async_remote_copy(src_ref=a, dst_ref=b, send_sem=ssem.at[n], recv_sem=rsem.at[n],
                                                    device_id=dev(d, 1 if up_ else 3), device_id_type=MESH))
        return res

    every, rest = (0, 1, 2, 3), (1, 2, 3)
    fin(own_line)
    pack_own()
    go(d2(0, (0,)))
    got(d1[0:3])
    go(passed(0))
    got(d1[3:6])
    go(passed(1))
    go(d2(1, (0,)))
    go(d2(2, (0,)))
    for c in range(NC):
        go(d2_own(c, (0,)))
    got(d1s)
    for q in range(2):
        got(passed(q))
    pack(0)
    go(d2(0, rest))
    go(d2_own(0, rest))

    own_x.wait()
    xcp.wait()
    fin(wshared)

    def shared(k, _):
        up(lambda: xs[k], 4)

        def store(n, v):
            acc[k, :, span(n, 256)] = v
        down(store, 4)
        return 0
    lax.fori_loop(0, 2, shared, 0)
    pcp = pltpu.make_async_remote_copy(src_ref=acc.at[1], dst_ref=prem, send_sem=tsem.at[2], recv_sem=tsem.at[3],
                                       device_id={"tp": 1 - tp}, device_id_type=MESH)
    pcp.start()
    wexp = weights(w1.at[0], w3.at[0], w2.at[0])
    go(wexp)

    pack(1)
    go(d2(1, rest))
    go(d2_own(1, rest))
    got(d2(0, every))
    fin(d2_own(0, every))
    go(d3(0))
    gone(d2(0, rest))
    pack(2)
    go(d2(2, rest))
    go(d2_own(2, rest))
    got(d2(1, every))
    fin(d2_own(1, every))
    go(d3(1))
    pcp.wait()
    acc[0] = acc[0] + (prem[...] + xs[0].astype(F32))
    fin(wexp)

    def first():
        load_e(0)

    def forward():
        got(d2(2, every))
        fin(d2_own(2, every))
        go(d3(2))

    def second():
        go(r3(0))
        go(r3_own(0))
        load_e(1)

    def third():
        go(r3(1))
        go(r3_own(1))
        load_e(2)
        gone(r3(0))
        fin(r3_own(0))

    def middle():
        got(r3(0))
        go(r2(0))
    experts(((0, first), (2, forward), (4, second), (8, third), (10, middle)))
    go(r3(2))
    go(r3_own(2))

    got(r3(1))
    fin(r3_own(1))
    go(r2(1))
    load_q(0)
    acc[1:4] = jnp.zeros((3, TOK, D), F32)
    add_all(0)
    got(r3(2))
    fin(r3_own(2))
    go(r2(2))
    load_q(1)
    add_all(1)
    for p in range(3):
        weigh(2, p, 2)
    load_q(2)
    low, high = r1(0), r1(1)
    for p in range(3):
        add(p, 2)
        low[p].start()
        high[p].start()

    def last(j, _):
        i = lax.rem(5 - j, 4)
        for p in range(3):
            weigh(2, p, i)
            add(p, i)

        @pl.when(j == 0)
        def _():
            go(r1(2))
        return 0
    lax.fori_loop(0, 3, last, 0)
    go(r1(3))
    res = local(acc.at[0], own, 0)
    res.start()
    for q in range(2):
        i = 1 + 2 * q
        via, on = r1(q), r1(4 + q)
        for p in range(3):
            via[p].wait_recv()
            acc[i, half[q], cols[p]] = acc[i, half[q], cols[p]] + mid[q, :, cols[p]]
            on[p].start()
    for q in range(2):
        gone(r1(q))
        fin(r1(2 + q))
        fin(r1(4 + q))
    res.wait()
    gone(d1 + d1s + passed(0) + passed(1) + d2(0, (0,)) + d2(1, every) + d2(2, every) + d3(0) + d3(1) + d3(2) + r3(1) + r3(2))
    for c in range(NC):
        gone(r2(c))


def _layer(x, idx, slot, g, ws1, ws3, ws2, w1, w3, w2):
    any_ = pl.BlockSpec(memory_space=pl.ANY)

    def blk(n):
        return jax.ShapeDtypeStruct((NC, 4, 4, 4, CH, n), BF)
    per = [blk(b) for _, b in COLS]
    shapes = [jax.ShapeDtypeStruct((TOK, D), F32)] + per + [blk(D)] + per + per
    shapes += [jax.ShapeDtypeStruct((2, TOK, D), F32)]
    scratch = [pltpu.VMEM((4, TOK, b), BF) for _, b in COLS]
    scratch += [pltpu.VMEM((K, TOK), jnp.int32), pltpu.VMEM((K, TOK), jnp.int32), pltpu.VMEM((K, TOK), F32)]
    scratch += [pltpu.VMEM((3, 4, 8, TOK), jnp.int32), pltpu.VMEM((3, 4, 8, TOK), F32)]
    scratch += [pltpu.VMEM((8, TOK), jnp.int32), pltpu.VMEM((8, TOK), F32)]
    scratch += [pltpu.VMEM((3, TOK, 3 * TOK), BF)]
    scratch += [pltpu.VMEM((2, 3, 4, 4, CH, b), BF) for _, b in COLS]
    scratch += [pltpu.VMEM((NC, 4, 4, CH, b), BF) for _, b in COLS]
    scratch += [pltpu.VMEM((4, 4, 4, CH, D), BF)]
    scratch += [pltpu.VMEM((4, 4, 4, CH, b), BF) for _, b in COLS]
    scratch += [
        pltpu.VMEM((2, 4, 4, 4, CH, D), BF),
        pltpu.VMEM((NT, D, 256), BF),
        pltpu.VMEM((8, F, 256), BF),
        pltpu.VMEM((TOK, F), BF),
        pltpu.VMEM((4, TOK, D), F32),
        pltpu.VMEM((2, TOK // 2, D), F32),
        pltpu.VMEM((2, TOK, D), BF),
        pltpu.VMEM((TOK, D), F32),
        pltpu.SemaphoreType.DMA((NSEM,)),
        pltpu.SemaphoreType.DMA((NSEM,)),
        pltpu.SemaphoreType.DMA((94,)),
        pltpu.SemaphoreType.DMA((2 * NT + 8,)),
        pltpu.SemaphoreType.DMA((4,)),
    ]
    res = pl.pallas_call(
        _kernel,
        out_shape=shapes,
        in_specs=[any_] * 10,
        out_specs=[any_] * len(shapes),
        scratch_shapes=scratch,
        compiler_params=pltpu.CompilerParams(collective_id=0, has_side_effects=True, vmem_limit_bytes=67043328),
    )(x, idx, slot, g, ws1, ws3, ws2, w1, w3, w2)
    own, others = res[0], res[-1]
    return (own + (others[0] + others[1])).astype(BF)


def solution(mesh):
    rows = P(("ep", "tp"), None)

    def body(x, idx, g, slot, ws1, ws3, ws2, w1, w3, w2):
        return _layer(x, idx.T, slot.T, g.T, ws1, ws3, ws2, w1, w3, w2)

    return jax.shard_map(
        body, mesh=mesh,
        in_specs=(rows, rows, rows, rows, P(None, "tp"), P(None, "tp"), P("tp", None),
                  P("ep", None, None), P("ep", None, None), P("ep", None, None)),
        out_specs=rows, check_vma=False)
```

```python
import jax
import jax.numpy as jnp
from jax import lax
from jax.experimental import pallas as pl
from jax.experimental.pallas import tpu as pltpu
from jax.sharding import PartitionSpec as P

MESH = pl.DeviceIdType.MESH
BF = jnp.bfloat16
F32 = jnp.float32

TOK = 256
D = 2048
F = 1408
K = 6
CAP = 48
CH = 16
NC = CAP // CH
NT = F // 128

COLS = ((0, 640), (640, 640), (1280, 768))
ORDER = ((0, 1, 2), (2, 0, 1), (1, 2, 0))
D1, PS, GS, R1, D2, D3, R3, R2 = range(8)
BASE = {D1: 0, PS: 9, GS: 18, D3: 27, R3: 54, R2: 81, D2: 108, R1: 216}
NSEM = 216 + 18 + 3


def _sem(stage, c, p, i, k):
    if stage == D2:
        return BASE[D2] + ((c * 3 + p) * 3 + i - 1) * 4 + k
    return BASE[stage] + (c * 3 + p) * 3 + i - 1


def _kernel(x, idx, slot, g, ws1, ws3, ws2, w1, w3, w2,
            own, sa, sb, sc, e, q3a, q3b, q3c, q2a, q2b, q2c, fr,
            la, lb, lc, iv, sv, gv, pt, gt, pm, gm, wt, pa, pb, pc, oa, ob, oc, ec, qa, qb, qc, r, w13, w2v, hid,
            acc, mid, xs, prem, ssem, rsem, lsem, wsem, tsem):
    ep = lax.axis_index("ep")
    tp = lax.axis_index("tp")
    z0, y0, x0 = ep // 16, lax.rem(ep // 4, 4), lax.rem(ep, 4)
    m = (z0 + tp * (y0 - z0), y0 + tp * (x0 - y0), x0 + tp * (z0 - x0))
    mz, my, mx = m
    kz, ky, kx = 16 - 12 * tp, 4 - 3 * tp, 1 + 15 * tp
    s = (sa, sb, sc)
    q3 = (q3a, q3b, q3c)
    q2 = (q2a, q2b, q2c)
    line = (la, lb, lc)
    pk = (pa, pb, pc)
    po = (oa, ob, oc)
    qv = (qa, qb, qc)
    cols = tuple(pl.ds(a, b) for a, b in COLS)

    AT = [[m[d] if i == 0 else lax.rem(m[d] + i, 4) for i in range(4)] for d in range(3)]
    DEV = [[kz * (AT[0][i] if d == 0 else mz) + ky * (AT[1][i] if d == 1 else my) + kx * (AT[2][i] if d == 2 else mx)
            for i in range(4)] for d in range(3)]

    def dev(d, i):
        return {"ep": DEV[d][i]}

    def at(d, i):
        return AT[d][i] if isinstance(i, int) else lax.rem(m[d] + i, 4)

    def src(d, i):
        return AT[d][(4 - i) % 4]

    def weights(u1, u3, u2):
        cps = []
        for n in range(NT):
            cps.append(pltpu.make_async_copy(u1.at[:, pl.ds(n * 128, 128)], w13.at[n, :, pl.ds(0, 128)], wsem.at[2 * n]))
            cps.append(pltpu.make_async_copy(u3.at[:, pl.ds(n * 128, 128)], w13.at[n, :, pl.ds(128, 128)], wsem.at[2 * n + 1]))
        for n in range(8):
            cps.append(pltpu.make_async_copy(u2.at[:, pl.ds(n * 256, 256)], w2v.at[n], wsem.at[2 * NT + n]))
        return cps

    small = [pltpu.make_async_copy(a, b, lsem.at[91 + n]) for n, (a, b) in enumerate(((idx, iv), (slot, sv), (g, gv)))]
    for c in small:
        c.start()

    bar = pltpu.get_barrier_semaphore()
    for d in range(3):
        for i in range(1, 4):
            pl.semaphore_signal(bar, inc=1, device_id=dev(d, i), device_id_type=MESH)
    pl.semaphore_signal(bar, inc=1, device_id={"tp": 1 - tp}, device_id_type=MESH)

    own_x = pltpu.make_async_copy(x, xs.at[0], lsem.at[0])
    own_x.start()
    own_line = [pltpu.make_async_copy(x.at[:, cols[p]], line[p].at[m[ORDER[p][0]]], lsem.at[1 + p]) for p in range(3)]
    for c in own_line:
        c.start()
    pm[...] = jnp.full((8, TOK), -1, jnp.int32)
    gm[...] = jnp.zeros((8, TOK), F32)
    for c in small:
        c.wait()
    pm[0:K, :] = jnp.where(sv[...] >= 0, iv[...] * CAP + sv[...], -1)
    gm[0:K, :] = gv[...]
    for d in range(3):
        pt[d, m[d]] = pm[...]
        gt[d, m[d]] = gm[...]
    pl.semaphore_wait(bar, 10)

    def remote(a, b, stage, c, p, i, where, k=0):
        n = _sem(stage, c, p, i, k)
        return pltpu.make_async_remote_copy(src_ref=a, dst_ref=b, send_sem=ssem.at[n], recv_sem=rsem.at[n],
                                            device_id=where, device_id_type=MESH)

    def local(a, b, n):
        return pltpu.make_async_copy(a, b, lsem.at[n])

    def go(cps):
        for cp in cps:
            cp.start()

    def fin(cps):
        for cp in cps:
            cp.wait()

    def got(cps):
        for cp in cps:
            cp.wait_recv()

    def gone(cps):
        for cp in cps:
            cp.wait_send()

    near = (1, 3, 2)

    half = (pl.ds(0, TOK // 2), pl.ds(TOK // 2, TOK // 2))
    d1 = []
    for i in (1, 3):
        for p in range(3):
            d = ORDER[p][0]
            d1.append(remote(x.at[:, cols[p]], line[p].at[m[d]], D1, 0, p, i, dev(d, i)))
    d1s = []
    for i in near:
        for p in range(3):
            d = ORDER[p][0]
            d1s.append(remote(pm, pt.at[d, m[d]], PS, 0, p, i, dev(d, i)))
            d1s.append(remote(gm, gt.at[d, m[d]], GS, 0, p, i, dev(d, i)))

    def passed(q):
        res = []
        for p in range(3):
            d = ORDER[p][0]
            v = line[p].at[AT[d][3 - 2 * q], half[q]]
            n = BASE[D1] + p * 3 + 1 if q == 0 else 234 + p
            res.append(pltpu.make_async_remote_copy(src_ref=v, dst_ref=v, send_sem=ssem.at[n], recv_sem=rsem.at[n],
                                                    device_id=dev(d, 1 + 2 * q), device_id_type=MESH))
        return res
    go(d1)
    go(d1s)
    xcp = pltpu.make_async_remote_copy(src_ref=x, dst_ref=xs.at[1], send_sem=tsem.at[0], recv_sem=tsem.at[1],
                                       device_id={"tp": 1 - tp}, device_id_type=MESH)
    xcp.start()
    wshared = weights(ws1, ws3, ws2)
    go(wshared)

    def tiles(count, unroll, f):
        def body(q, _):
            for u in range(unroll):
                f(q * unroll + u)
            return 0
        whole = count // unroll
        if whole == 1:
            body(0, 0)
        else:
            lax.fori_loop(0, whole, body, 0)
        for n in range(whole * unroll, count):
            f(n)

    def span(n, w):
        return pl.ds(n * w if isinstance(n, int) else pl.multiple_of(n * w, w), w)

    def up(rows, unroll):
        def f(n):
            ab = jnp.dot(rows(), w13[n], preferred_element_type=F32)
            hid[:, span(n, 128)] = (jax.nn.silu(ab[:, :128]) * ab[:, 128:]).astype(BF)
        tiles(NT, unroll, f)

    def down(store, unroll):
        tiles(8, unroll, lambda n: store(n, jnp.dot(hid[...], w2v[n], preferred_element_type=F32)))

    ri = lax.broadcasted_iota(jnp.int32, (TOK, TOK), 0)
    ra, rb, rs = ri // 64, (ri // 16) % 4, ri % 16
    ex = (mz * kz + ra * ky + rb * kx, ra * kz + rb * ky + mx * kx, rb * kz + my * ky + ra * kx)
    base = tuple(v * CAP + rs for v in ex)

    def picked(c, p, v):
        ps = pt[ORDER[p][0], v] - c * CH
        hit = ps[0:1, :] == base[p]
        for j in range(1, K):
            hit = hit | (ps[j:j + 1, :] == base[p])
        oh = jnp.where(hit, 1.0, 0.0).astype(BF)
        w = jnp.dot(oh, line[p][v], preferred_element_type=F32).astype(BF)
        return w.reshape(4, 4, CH, COLS[p][1])

    def pack(c):
        def body(k, _):
            for p in range(3):
                pk[p][c % 2 if isinstance(c, int) else lax.rem(c, 2), k] = picked(c, p, at(ORDER[p][0], k + 1))
            return 0
        lax.fori_loop(0, 3, body, 0)

    def pack_own():
        def body(c, _):
            for p in range(3):
                po[p][c] = picked(c, p, m[ORDER[p][0]])
            return 0
        lax.fori_loop(0, NC, body, 0)

    def packed(c, p, k):
        return po[p].at[c] if k == 0 else pk[p].at[c % 2, k - 1]

    def s_dst(p, c, b, v):
        return s[p].at[c, :, b, v] if p == 1 else s[p].at[c, :, v, b]

    def d2(c, ks):
        res = []
        for k in ks:
            for i in near:
                for p in range(3):
                    d = ORDER[p][1]
                    res.append(remote(packed(c, p, k).at[at(d, i)], s_dst(p, c, m[d], at(ORDER[p][0], k)),
                                      D2, c, p, i, dev(d, i), k))
        return res

    def d2_own(c, ks):
        res = []
        for k in ks:
            for p in range(3):
                v = m[ORDER[p][1]]
                res.append(local(packed(c, p, k).at[v], s_dst(p, c, v, at(ORDER[p][0], k)), 55 + (c * 3 + p) * 4 + k))
        return res

    def e_at(buf, p, v):
        if p == 0:
            return buf.at[:, :, v, :, cols[0]]
        if p == 1:
            return buf.at[:, v, :, :, cols[1]]
        return buf.at[v, :, :, :, cols[2]]

    def d3(c):
        res = []
        for i in near:
            for p in range(3):
                d = ORDER[p][2]
                res.append(remote(s[p].at[c, at(d, i)], e_at(e.at[c], p, m[d]), D3, c, p, i, dev(d, i)))
        return res

    def load_e(c):
        cps = [local(s[p].at[c, m[ORDER[p][2]]], e_at(ec, p, m[ORDER[p][2]]), 13 + p * 4) for p in range(3)]
        go(cps)
        arrived = d3(c)
        for q, i in enumerate(near):
            for p in range(3):
                arrived[q * 3 + p].wait_recv()
                v = src(ORDER[p][2], i)
                cp = local(e_at(e.at[c], p, v), e_at(ec, p, v), 13 + p * 4 + i)
                cp.start()
                cps.append(cp)
        fin(cps)

    def experts(events):
        def body(b, _):
            for at_b, event in events:
                pl.when(b == at_b)(event)
            z = lax.rem(b, 4)
            up(lambda: ec[z].reshape(TOK, D), NT)

            def store(n, v):
                r[lax.rem(b // 4, 2), z, :, :, :, span(n, 256)] = v.astype(BF).reshape(4, 4, CH, 256)
            down(store, 8)
            return 0
        lax.fori_loop(0, 4 * NC, body, 0)

    def r3(c):
        res = []
        for i in near:
            for p in range(3):
                d = ORDER[p][2]
                res.append(remote(e_at(r.at[c % 2], p, at(d, i)), q3[p].at[c, m[d]], R3, c, p, i, dev(d, i)))
        return res

    def r3_own(c):
        return [local(e_at(r.at[c % 2], p, m[ORDER[p][2]]), q3[p].at[c, m[ORDER[p][2]]], 25 + c * 3 + p) for p in range(3)]

    def q3_at(p, c, v):
        return q3[p].at[c, :, v] if p == 1 else q3[p].at[c, :, :, v]

    def q2_at(p, c, v):
        return q2[p].at[c, :, v] if p == 2 else q2[p].at[c, v]

    def r2(c):
        res = []
        for i in near:
            for p in range(3):
                d = ORDER[p][1]
                res.append(remote(q3_at(p, c, at(d, i)), q2_at(p, c, m[d]), R2, c, p, i, dev(d, i)))
        return res

    def load_q(c):
        cps = []
        for p in range(3):
            w = m[ORDER[p][1]]
            cps.append(local(q3_at(p, c, w), qv[p].at[w], 34 + p * 4))
        go(cps)
        arrived = r2(c)
        for q, i in enumerate(near):
            for p in range(3):
                arrived[q * 3 + p].wait_recv()
                w = src(ORDER[p][1], i)
                cp = local(q2_at(p, c, w), qv[p].at[w], 34 + p * 4 + i)
                cp.start()
                cps.append(cp)
        fin(cps)

    def weigh(c, p, i):
        d = ORDER[p][0]
        v = at(d, i)
        ps = pt[d, v] - c * CH
        gs = gt[d, v]
        w = jnp.zeros((TOK, TOK), F32)
        for j in range(K):
            w = w + jnp.where(ps[j:j + 1, :] == base[p], gs[j:j + 1, :], 0.0)
        w1_ = w.astype(BF)
        t = w - w1_.astype(F32)
        w2_ = t.astype(BF)
        w3_ = (t - w2_.astype(F32)).astype(BF)
        wt[p, :, 0:TOK] = w1_
        wt[p, :, TOK:2 * TOK] = w2_
        wt[p, :, 2 * TOK:3 * TOK] = w3_

    def add(p, i):
        rows = qv[p][:, :, at(ORDER[p][0], i)].reshape(TOK, COLS[p][1])
        y = lax.dot_general(wt[p], rows, (((0,), (0,)), ((), ())), preferred_element_type=F32)
        y = (y[2 * TOK:] + y[TOK:2 * TOK]) + y[:TOK]
        acc[i, :, cols[p]] = acc[i, :, cols[p]] + y

    def add_all(c):
        def body(i, _):
            for p in range(3):
                weigh(c, p, i)
                add(p, i)
            return 0
        lax.fori_loop(0, 4, body, 0)

    def r1(q):
        res = []
        for p in range(3):
            d = ORDER[p][0]
            n = BASE[R1] + p * 6 + q
            up_ = q % 2 == 0
            if q < 2:
                a, b = acc.at[2, half[q], cols[p]], mid.at[q, :, cols[p]]
            else:
                rows = half[{2: 1, 3: 0, 4: 0, 5: 1}[q]]
                a, b = acc.at[1 if up_ else 3, rows, cols[p]], fr.at[0 if q < 4 else 1, rows, cols[p]]
            res.append(pltpu.make_async_remote_copy(src_ref=a, dst_ref=b, send_sem=ssem.at[n], recv_sem=rsem.at[n],
                                                    device_id=dev(d, 1 if up_ else 3), device_id_type=MESH))
        return res

    every, rest = (0, 1, 2, 3), (1, 2, 3)
    fin(own_line)
    pack_own()
    go(d2(0, (0,)))
    got(d1[0:3])
    go(passed(0))
    got(d1[3:6])
    go(passed(1))
    go(d2(1, (0,)))
    go(d2(2, (0,)))
    for c in range(NC):
        go(d2_own(c, (0,)))
    got(d1s)
    for q in range(2):
        got(passed(q))
    pack(0)
    go(d2(0, rest))
    go(d2_own(0, rest))

    own_x.wait()
    xcp.wait()
    fin(wshared)

    def shared(k, _):
        up(lambda: xs[k], 4)

        def store(n, v):
            acc[k, :, span(n, 256)] = v
        down(store, 4)
        return 0
    lax.fori_loop(0, 2, shared, 0)
    pcp = pltpu.make_async_remote_copy(src_ref=acc.at[1], dst_ref=prem, send_sem=tsem.at[2], recv_sem=tsem.at[3],
                                       device_id={"tp": 1 - tp}, device_id_type=MESH)
    pcp.start()
    wexp = weights(w1.at[0], w3.at[0], w2.at[0])
    go(wexp)

    pack(1)
    go(d2(1, rest))
    go(d2_own(1, rest))
    got(d2(0, every))
    fin(d2_own(0, every))
    go(d3(0))
    gone(d2(0, rest))
    pack(2)
    go(d2(2, rest))
    go(d2_own(2, rest))
    got(d2(1, every))
    fin(d2_own(1, every))
    go(d3(1))
    pcp.wait()
    acc[0] = acc[0] + (prem[...] + xs[0].astype(F32))
    fin(wexp)

    def first():
        load_e(0)

    def forward():
        got(d2(2, every))
        fin(d2_own(2, every))
        go(d3(2))

    def second():
        go(r3(0))
        go(r3_own(0))
        load_e(1)

    def third():
        go(r3(1))
        go(r3_own(1))
        load_e(2)
        gone(r3(0))
        fin(r3_own(0))

    def middle():
        got(r3(0))
        go(r2(0))
    experts(((0, first), (2, forward), (4, second), (8, third), (9, middle)))
    go(r3(2))
    go(r3_own(2))

    got(r3(1))
    fin(r3_own(1))
    go(r2(1))
    load_q(0)
    acc[1:4] = jnp.zeros((3, TOK, D), F32)
    add_all(0)
    got(r3(2))
    fin(r3_own(2))
    go(r2(2))
    load_q(1)
    add_all(1)
    for p in range(3):
        weigh(2, p, 2)
    load_q(2)
    low, high = r1(0), r1(1)
    for p in range(3):
        add(p, 2)
        low[p].start()
        high[p].start()

    def last(j, _):
        i = lax.rem(5 - j, 4)
        for p in range(3):
            weigh(2, p, i)
            add(p, i)

        @pl.when(j == 0)
        def _():
            go(r1(2))
        return 0
    lax.fori_loop(0, 3, last, 0)
    go(r1(3))
    for q in range(2):
        i = 1 + 2 * q
        via, on = r1(q), r1(4 + q)
        for p in range(3):
            via[p].wait_recv()
            acc[i, half[q], cols[p]] = acc[i, half[q], cols[p]] + mid[q, :, cols[p]]
            on[p].start()
    got(r1(2) + r1(3))
    res = local(fr.at[0], prem, 0)
    res.start()
    res.wait()
    acc[0] = acc[0] + prem[...]
    res = local(acc.at[0], own, 1)
    res.start()
    for q in range(2):
        gone(r1(q))
        gone(r1(2 + q))
        fin(r1(4 + q))
    res.wait()
    gone(d1 + d1s + passed(0) + passed(1) + d2(0, (0,)) + d2(1, every) + d2(2, every) + d3(0) + d3(1) + d3(2) + r3(1) + r3(2))
    for c in range(NC):
        gone(r2(c))


def _layer(x, idx, slot, g, ws1, ws3, ws2, w1, w3, w2):
    any_ = pl.BlockSpec(memory_space=pl.ANY)

    def blk(n):
        return jax.ShapeDtypeStruct((NC, 4, 4, 4, CH, n), BF)
    per = [blk(b) for _, b in COLS]
    shapes = [jax.ShapeDtypeStruct((TOK, D), F32)] + per + [blk(D)] + per + per
    shapes += [jax.ShapeDtypeStruct((2, TOK, D), F32)]
    scratch = [pltpu.VMEM((4, TOK, b), BF) for _, b in COLS]
    scratch += [pltpu.VMEM((K, TOK), jnp.int32), pltpu.VMEM((K, TOK), jnp.int32), pltpu.VMEM((K, TOK), F32)]
    scratch += [pltpu.VMEM((3, 4, 8, TOK), jnp.int32), pltpu.VMEM((3, 4, 8, TOK), F32)]
    scratch += [pltpu.VMEM((8, TOK), jnp.int32), pltpu.VMEM((8, TOK), F32)]
    scratch += [pltpu.VMEM((3, TOK, 3 * TOK), BF)]
    scratch += [pltpu.VMEM((2, 3, 4, 4, CH, b), BF) for _, b in COLS]
    scratch += [pltpu.VMEM((NC, 4, 4, CH, b), BF) for _, b in COLS]
    scratch += [pltpu.VMEM((4, 4, 4, CH, D), BF)]
    scratch += [pltpu.VMEM((4, 4, 4, CH, b), BF) for _, b in COLS]
    scratch += [
        pltpu.VMEM((2, 4, 4, 4, CH, D), BF),
        pltpu.VMEM((NT, D, 256), BF),
        pltpu.VMEM((8, F, 256), BF),
        pltpu.VMEM((TOK, F), BF),
        pltpu.VMEM((4, TOK, D), F32),
        pltpu.VMEM((2, TOK // 2, D), F32),
        pltpu.VMEM((2, TOK, D), BF),
        pltpu.VMEM((TOK, D), F32),
        pltpu.SemaphoreType.DMA((NSEM,)),
        pltpu.SemaphoreType.DMA((NSEM,)),
        pltpu.SemaphoreType.DMA((94,)),
        pltpu.SemaphoreType.DMA((2 * NT + 8,)),
        pltpu.SemaphoreType.DMA((4,)),
    ]
    res = pl.pallas_call(
        _kernel,
        out_shape=shapes,
        in_specs=[any_] * 10,
        out_specs=[any_] * len(shapes),
        scratch_shapes=scratch,
        compiler_params=pltpu.CompilerParams(collective_id=0, has_side_effects=True, vmem_limit_bytes=67043328),
    )(x, idx, slot, g, ws1, ws3, ws2, w1, w3, w2)
    own, others = res[0], res[-1]
    return (own + others[1]).astype(BF)


def solution(mesh):
    rows = P(("ep", "tp"), None)

    def body(x, idx, g, slot, ws1, ws3, ws2, w1, w3, w2):
        return _layer(x, idx.T, slot.T, g.T, ws1, ws3, ws2, w1, w3, w2)

    return jax.shard_map(
        body, mesh=mesh,
        in_specs=(rows, rows, rows, rows, P(None, "tp"), P(None, "tp"), P("tp", None),
                  P("ep", None, None), P("ep", None, None), P("ep", None, None)),
        out_specs=rows, check_vma=False)
```
